64 devices in a mesh: rep: 8 (over x, y, core), dp: 8 (over z).
Axes of the slice: x: 2, y: 2, z: 8, core: 2. Of those that a mesh axis runs over, the one named last changes fastest.
The devices are a block of a 4x4x8 slice.
Arguments:
- x: bfloat16 [64, 4096, 512], P(('rep', 'dp')), parts along dimension 0
- dy: bfloat16 [64, 4096, 512], P(('rep', 'dp')), parts along dimension 0
- w_gate: bfloat16 [2, 512, 2048], replicated
- w_up: bfloat16 [2, 512, 2048], replicated
- w_down: bfloat16 [2, 2048, 512], replicated
- m_w_gate: float32 [2, 512, 2048], replicated
- m_w_up: float32 [2, 512, 2048], replicated
- m_w_down: float32 [2, 2048, 512], replicated
- v_w_gate: float32 [2, 512, 2048], replicated
- v_w_up: float32 [2, 512, 2048], replicated
- v_w_down: float32 [2, 2048, 512], replicated
Outputs:
- output 1: bfloat16 [16, 512, 2048], P('rep'), parts along dimension 0
- output 2: bfloat16 [16, 512, 2048], P('rep'), parts along dimension 0
- output 3: bfloat16 [16, 2048, 512], P('rep'), parts along dimension 0
- output 4: float32 [16, 512, 2048], P('rep'), parts along dimension 0
- output 5: float32 [16, 512, 2048], P('rep'), parts along dimension 0
- output 6: float32 [16, 2048, 512], P('rep'), parts along dimension 0
- output 7: float32 [16, 512, 2048], P('rep'), parts along dimension 0
- output 8: float32 [16, 512, 2048], P('rep'), parts along dimension 0
- output 9: float32 [16, 2048, 512], P('rep'), parts along dimension 0
There are 8 independent parts. The reference program is written for one: setup_inputs(seed, part) draws one part's arguments, and reference() takes and returns one part's arrays. A program takes and returns all parts, laid end to end along the dimension named above; an argument that names none is the same for every part.
All inputs are finite; a program needn't handle non-finite values.
Results may differ from the reference program's by a relative error of at most 0.022.
Values are sent between devices in bfloat16 or wider.
A program may use at most 768 MiB of HBM per device.

```python
import jax
import jax.numpy as jnp
from jax import lax

SEQUENCES = 8
TOKENS = 4096
D = 512
FF = 2048
LAYERS = 2
NAMES = ("w_gate", "w_up", "w_down")
SHAPES = {"w_gate": (LAYERS, D, FF), "w_up": (LAYERS, D, FF), "w_down": (LAYERS, FF, D)}


def bump(key, n, height):
    away = (jnp.arange(n, dtype=jnp.int32) - jax.random.randint(key, (), 0, n, jnp.int32)) % n
    return jnp.where(away < n // 8, height, 1.0)


def together(key, own, strength):
    shared = jax.random.normal(key, own.shape[1:], jnp.float32)
    return (own + strength * shared) * lax.rsqrt(1 + strength * strength)


def setup_inputs(seed: int = 0, part: int = 0) -> dict:
    kx, kdy, ka, kb, kz, kf, kh, kl, *keys = jax.random.split(jax.random.key(seed), 8 + 3 * len(NAMES))
    kx, kdy, ka, kb = (jax.random.fold_in(k, part) for k in (kx, kdy, ka, kb))
    kw, km, kv = (keys[i::3] for i in range(3))
    shape = (SEQUENCES, TOKENS, D)
    much_x, much_dy = jax.random.uniform(kz, (2,), jnp.float32, 0.0, 1.0)
    loud = 2.0 ** jax.random.uniform(jax.random.fold_in(kz, 1), (), jnp.float32, -1.0, 2.0)
    layers = 2.0 ** jax.random.uniform(kl, (LAYERS, 1, 1), jnp.float32, -1.0, 1.0)
    x = together(ka, jax.random.normal(kx, shape, jnp.float32), much_x) * bump(kf, D, 4.0)
    dy = together(kb, jax.random.normal(kdy, shape, jnp.float32), much_dy)
    drawn = {"x": x.astype(jnp.bfloat16), "dy": (loud * dy * (SEQUENCES * TOKENS) ** -0.5).astype(jnp.bfloat16)}
    for key, name in zip(kw, NAMES, strict=True):
        w = jax.random.normal(key, SHAPES[name], jnp.float32) * SHAPES[name][1] ** -0.5
        drawn[name] = (w * {"w_gate": 1.0, "w_up": bump(kh, FF, 4.0), "w_down": layers}[name]).astype(jnp.bfloat16)
    for key, name in zip(km, NAMES, strict=True):
        drawn[f"m_{name}"] = 0.1 * jax.random.normal(key, SHAPES[name], jnp.float32)
    for key, name in zip(kv, NAMES, strict=True):
        drawn[f"v_{name}"] = jax.random.uniform(key, SHAPES[name], jnp.float32, 0.005, 0.015)
    return drawn


def matmul(a, w):
    return jnp.dot(a, w, preferred_element_type=jnp.float32).astype(jnp.bfloat16)


def normed(h):
    wide = h.astype(jnp.float32)
    scale = lax.rsqrt(jnp.mean(wide**2, -1, keepdims=True) + 1e-6)
    return (wide * scale).astype(jnp.bfloat16)


def layer(h, w):
    a = normed(h)
    gate = jnp.dot(a, w["w_gate"], preferred_element_type=jnp.float32)
    up = jnp.dot(a, w["w_up"], preferred_element_type=jnp.float32)
    return h + matmul((jax.nn.silu(gate) * up).astype(jnp.bfloat16), w["w_down"])


def adamw(w, m, v, g):
    m = 0.9 * m + 0.1 * g
    v = 0.95 * v + 0.05 * g * g
    step = m * lax.rsqrt(v + 1e-8) + 0.1 * w
    return (w - 0.02 * step).astype(jnp.bfloat16), m, v


def clipped(gradients, sum_of_squares, count):
    factor = jnp.minimum(1.0, 0.5 * lax.rsqrt(sum_of_squares / count + 1e-30))
    return [g * factor for g in gradients]


def stack(weights, h):
    return lax.scan(lambda h, w: (layer(h, w), None), h, weights)[0]


def reference(x, dy, w_gate, w_up, w_down, m_w_gate, m_w_up, m_w_down, v_w_gate, v_w_up, v_w_down):
    weights = dict(zip(NAMES, (w_gate, w_up, w_down), strict=True))

    def take(so_far, sequence):
        h, by_y = sequence
        _, back = jax.vjp(lambda w: stack(w, h), weights)
        return jax.tree.map(lambda total, term: total + term.astype(jnp.float32), so_far, back(by_y)[0]), None

    none_yet = {name: jnp.zeros(w.shape, jnp.float32) for name, w in weights.items()}
    by_weights, _ = lax.scan(take, none_yet, (x, dy))
    gradients = [by_weights[name].astype(jnp.bfloat16).astype(jnp.float32) for name in NAMES]
    gradients = clipped(gradients, sum(jnp.sum(g * g) for g in gradients), sum(g.size for g in gradients))
    new = [
        adamw(w.astype(jnp.float32), m, v, g)
        for w, m, v, g in zip((w_gate, w_up, w_down), (m_w_gate, m_w_up, m_w_down), (v_w_gate, v_w_up, v_w_down), gradients, strict=True)
    ]
    return tuple(one[which] for which in range(3) for one in new)
```

```python
import functools

import jax
import jax.numpy as jnp
from jax import lax
from jax.experimental import pallas as pl
from jax.experimental.pallas import tpu as pltpu
from jax.sharding import PartitionSpec as P

F32, BF16 = jnp.float32, jnp.bfloat16
AXIS = "dp"
TILE = 512
CHUNK = 256
VMEM_LIMIT = 67043328


def mm(a, b):
    return jnp.dot(a, b, preferred_element_type=F32)


def mm_nt(a, b):
    return lax.dot_general(a, b, (((1,), (1,)), ((), ())), preferred_element_type=F32)


def mm_tn(a, b):
    return lax.dot_general(a, b, (((0,), (0,)), ((), ())), preferred_element_type=F32)


def sigmoid(x):
    return 0.5 * jnp.tanh(0.5 * x) + 0.5


def normed(wide):
    scale = lax.rsqrt(jnp.mean(wide * wide, -1, keepdims=True) + 1e-6)
    return (wide * scale).astype(BF16)


def gradients_body(n, x_hbm, dy_hbm, wg_hbm, wu_hbm, wd_hbm, full_hbm, own_hbm, squares_ref,
                   a0, a0t, a1, a1t, dy, h1, acc, w0g, w0u, w0d, w1, w1d, act, dgu, accd, accgu, grads, slots, sums, squares,
                   first_sem, w1_sem, rs_send, rs_recv, ag_send, ag_recv, sq_send, sq_recv, full_sem, own_sem):
    tokens, d = h1.shape
    ff = w0d.shape[0]
    tiles, chunks = tokens // TILE, ff // CHUNK
    groups = 2 * chunks
    hops = n // 2
    shard_rows = grads.shape[1] // n
    half = shard_rows // 2
    me = lax.axis_index(AXIS)
    to = (lax.rem(me + 1, n), lax.rem(me + n - 1, n))

    def rows(t):
        return pl.ds(pl.multiple_of(t * TILE, TILE), TILE)

    def cols(c):
        return pl.ds(pl.multiple_of(c * CHUNK, CHUNK), CHUNK)

    def shard(away):
        return pl.multiple_of(lax.rem(me + away + n, n) * shard_rows, shard_rows)

    def remote(src, dst, send, recv, way):
        return pltpu.make_async_remote_copy(src_ref=src, dst_ref=dst, send_sem=send, recv_sem=recv, device_id={AXIS: to[way]}, device_id_type=pl.DeviceIdType.MESH)

    def rs_copy(s, g, way):
        p = lax.rem(g, 2)
        if s == 1:
            part = pl.ds(way * half, half)
            src, dst = grads.at[g, pl.ds(shard(hops) + way * half, half)], slots.at[way, 0, p, part]
        else:
            src, dst = sums.at[way, s - 2, p], slots.at[way, s - 1, p]
        return remote(src, dst, rs_send.at[way, s - 1, p], rs_recv.at[way, s - 1, p], way)

    def rs_add(s, g):
        p = lax.rem(g, 2)
        for way in range(2):
            own = grads[g, pl.ds(shard((1 - 2 * way) * (hops + 1 - s)), shard_rows)]
            if s == 2:
                here = slice(way * half, way * half + half)
                there = slice(half - way * half, shard_rows - way * half)
                sums[way, 0, p, there] = own[there]
                sums[way, 0, p, here] = (slots[way, 0, p, here].astype(F32) + own[here].astype(F32)).astype(BF16)
            else:
                sums[way, s - 2, p] = (slots[way, s - 2, p].astype(F32) + own.astype(F32)).astype(BF16)

    def rs_final(g):
        p = lax.rem(g, 2)
        mine = pl.ds(shard(0), shard_rows)
        total = slots[0, hops - 1, p].astype(F32) + slots[1, hops - 1, p].astype(F32) + grads[g, mine].astype(F32)
        total = total.astype(BF16)
        grads[g, mine] = total
        wide = total.astype(F32)
        squares[0] += jnp.sum((wide * wide).reshape(shard_rows // 8, 8, CHUNK), axis=0)

    def ag_copies(k, whole):
        pair, j = k // hops, lax.rem(k, hops)
        copies = []
        for b in range(2):
            for way in range(2):
                at = shard((2 * way - 1) * j)
                part = pl.ds(at, shard_rows) if whole else pl.ds(at + way * half, half)
                ref = grads.at[2 * pair + b, part]
                copies.append(remote(ref, ref, ag_send.at[way, j, b], ag_recv.at[way, j, b], way))
        return copies

    def full_copy(pair):
        return pltpu.make_async_copy(grads.at[pl.ds(2 * pair, 2)], full_hbm.at[pl.ds(2 * pair, 2)], full_sem.at[pair])

    def own_copy(g):
        return pltpu.make_async_copy(grads.at[g, pl.ds(shard(0), shard_rows)], own_hbm.at[g - chunks], own_sem.at[g - chunks])

    gathers = hops * (chunks // 2)

    def tick(t):
        def group(g, f):
            pl.when((g >= 0) & (g < groups))(functools.partial(f, g))

        def arrived(s, g):
            for way in range(2):
                rs_copy(s, g, way).wait()

        def add(s, g):
            arrived(s - 1, g)
            rs_add(s, g)

        def final(g):
            arrived(hops, g)
            rs_final(g)

        def send(s, g):
            for way in range(2):
                rs_copy(s, g, way).start()

        for s in range(hops, 1, -1):
            group(t - s, functools.partial(add, s))
        group(t - hops - 1, final)
        for s in range(hops, 0, -1):
            group(t - s, functools.partial(send, s))

        k = t - hops - 2
        for whole in (True, False):
            last = hops - 1

            @pl.when((k >= 1) & (k <= gathers) & ((lax.rem(k - 1 + hops, hops) < last) == whole))
            def _():
                for copy in ag_copies(k - 1, whole):
                    copy.wait()

        for whole in (True, False):
            last = hops - 1

            @pl.when((k >= 0) & (k < gathers) & ((lax.rem(k + 2 * hops, hops) < last) == whole))
            def _():
                for copy in ag_copies(k, whole):
                    copy.start()

        @pl.when((k >= hops) & (k <= gathers) & (lax.rem(k + 2 * hops, hops) == 0))
        def _():
            full_copy(k // hops - 1).start()

        g = t - hops - 2

        @pl.when((g >= chunks) & (g < groups))
        def _():
            own_copy(g).start()

    def w1_copies(c):
        slot = lax.rem(c, 2)
        return (
            pltpu.make_async_copy(wg_hbm.at[1, :, cols(c)], w1.at[slot, :, pl.ds(0, CHUNK)], w1_sem.at[slot, 0]),
            pltpu.make_async_copy(wu_hbm.at[1, :, cols(c)], w1.at[slot, :, pl.ds(CHUNK, CHUNK)], w1_sem.at[slot, 1]),
            pltpu.make_async_copy(wd_hbm.at[1, cols(c), :], w1d.at[slot], w1_sem.at[slot, 2]),
        )

    squares[...] = jnp.zeros_like(squares)
    barrier = pltpu.get_barrier_semaphore()
    for away in range(1, n):
        pl.semaphore_signal(barrier, inc=1, device_id={AXIS: lax.rem(me + away, n)}, device_id_type=pl.DeviceIdType.MESH)

    first = (
        pltpu.make_async_copy(x_hbm.at[0], h1, first_sem.at[0]),
        pltpu.make_async_copy(wg_hbm.at[0], w0g, first_sem.at[1]),
        pltpu.make_async_copy(wu_hbm.at[0], w0u, first_sem.at[2]),
        pltpu.make_async_copy(wd_hbm.at[0], w0d, first_sem.at[3]),
        pltpu.make_async_copy(dy_hbm.at[0], dy, first_sem.at[4]),
    )
    for copy in first + w1_copies(0) + w1_copies(1):
        copy.start()

    def norm0(t):
        a = normed(h1[rows(t), :].astype(F32))
        a0[rows(t), :] = a
        a0t[:, rows(t)] = a.T

    first[0].wait()
    norm0(0)
    accd[...] = jnp.zeros_like(accd)
    accgu[...] = jnp.zeros_like(accgu)
    for copy in first[1:4]:
        copy.wait()

    def forward(t, _):
        a = a0[rows(t), :]

        @pl.when(t + 1 < tiles)
        def _():
            norm0(t + 1)

        for c in range(chunks):
            s = pl.ds(c * CHUNK, CHUNK)
            gate, up = mm(a, w0g[:, s]), mm(a, w0u[:, s])
            grads[c, :TILE, :] = (gate * sigmoid(gate) * up).astype(BF16)
        acc[rows(t), :] = jnp.zeros((TILE, d), F32)
        out = mm(grads[0, :TILE, :], w0d[:CHUNK, :])
        for c in range(1, chunks):
            out += mm(grads[c, :TILE, :], w0d[c * CHUNK : (c + 1) * CHUNK, :])
        h = (h1[rows(t), :].astype(F32) + out.astype(BF16).astype(F32)).astype(BF16)
        h1[rows(t), :] = h
        a = normed(h.astype(F32))
        a1[rows(t), :] = a
        a1t[:, rows(t)] = a.T
        return 0

    lax.fori_loop(0, tiles, forward, 0)
    first[4].wait()
    pl.semaphore_wait(barrier, n - 1)

    def elementwise(gate, up, dact, b):
        s = sigmoid(gate)
        p = gate * s
        act[b] = (p * up).astype(BF16)
        dact = dact.astype(BF16).astype(F32)
        dgu[b, :, CHUNK:] = (dact * p).astype(BF16)
        dgu[b, :, :CHUNK] = (dact * up * (s + p * (1.0 - s))).astype(BF16)

    def finish(g):
        rd, rf = d // n, CHUNK // n
        for r in range(n):
            at = r * shard_rows
            grads[g, at : at + rd, :] = accgu[r * rd : (r + 1) * rd, :CHUNK].astype(BF16)
            grads[g, at + rd : at + 2 * rd, :] = accgu[r * rd : (r + 1) * rd, CHUNK:].astype(BF16)
            for q in range(d // CHUNK):
                grads[g, at + 2 * rd + q * rf : at + 2 * rd + (q + 1) * rf, :] = accd[r * rf : (r + 1) * rf, q * CHUNK : (q + 1) * CHUNK].astype(BF16)
        accd[...] = jnp.zeros_like(accd)
        accgu[...] = jnp.zeros_like(accgu)

    total = chunks * tiles

    def front1(i):
        c, t, b = i // tiles, lax.rem(i, tiles), lax.rem(i, 2)
        slot = lax.rem(c, 2)
        a = a1[rows(t), :]
        elementwise(mm(a, w1[slot, :, :CHUNK]), mm(a, w1[slot, :, CHUNK:]), mm_nt(dy[rows(t), :], w1d[slot]), b)

    def back1(i):
        c, t, b = i // tiles, lax.rem(i, tiles), lax.rem(i, 2)
        accd[...] += mm_tn(act[b], dy[rows(t), :])
        accgu[...] += mm(a1t[:, rows(t)], dgu[b])
        acc[rows(t), :] += mm_nt(dgu[b], w1[lax.rem(c, 2)])

    def layer1(i, _):
        c, t = i // tiles, lax.rem(i, tiles)

        @pl.when((t == tiles - 1) & (c + 1 < chunks))
        def _():
            for copy in w1_copies(c + 1):
                copy.wait()

        front1(jnp.minimum(i + 1, total - 1))
        back1(i)

        @pl.when(t == tiles - 1)
        def _():
            finish(c)

            @pl.when(c + 2 < chunks)
            def _():
                for copy in w1_copies(c + 2):
                    copy.start()

            tick(c + 1)

        return 0

    for copy in w1_copies(0):
        copy.wait()
    front1(0)
    lax.fori_loop(0, total, layer1, 0)

    def between(t, _):
        da = acc[rows(t), :].astype(BF16).astype(F32)
        wide = h1[rows(t), :].astype(F32)
        scale = lax.rsqrt(jnp.mean(wide * wide, -1, keepdims=True) + 1e-6)
        along = jnp.sum(da * wide, -1, keepdims=True) * (scale * scale * scale / d)
        through = (da * scale - wide * along).astype(BF16).astype(F32)
        dy[rows(t), :] = (dy[rows(t), :].astype(F32) + through).astype(BF16)
        return 0

    lax.fori_loop(0, tiles, between, 0)

    def front0(i):
        c, t, b = i // tiles, lax.rem(i, tiles), lax.rem(i, 2)
        a = a0[rows(t), :]
        elementwise(mm(a, w0g[:, cols(c)]), mm(a, w0u[:, cols(c)]), mm_nt(dy[rows(t), :], w0d[cols(c), :]), b)

    def layer0(i, _):
        c, t, b = i // tiles, lax.rem(i, tiles), lax.rem(i, 2)
        front0(jnp.minimum(i + 1, total - 1))
        accd[...] += mm_tn(act[b], dy[rows(t), :])
        accgu[...] += mm(a0t[:, rows(t)], dgu[b])

        @pl.when(t == tiles - 1)
        def _():
            finish(chunks + c)
            tick(chunks + c + 1)

        return 0

    front0(0)
    lax.fori_loop(0, total, layer0, 0)

    def sq_copy(away, mine):
        q = me if mine else lax.rem(me + away, n)
        return pltpu.make_async_remote_copy(
            src_ref=squares.at[0], dst_ref=squares.at[1 + q], send_sem=sq_send.at[away - 1], recv_sem=sq_recv.at[q],
            device_id={AXIS: lax.rem(me + away, n)}, device_id_type=pl.DeviceIdType.MESH)

    last = max(groups + hops + 1, gathers + hops + 2)

    def drain(t, _):
        tick(t)

        @pl.when(t == groups + hops)
        def _():
            for away in range(1, n):
                sq_copy(away, True).start()

        return 0

    lax.fori_loop(groups + 1, last + 1, drain, 0)
    for away in range(1, n):
        sq_copy(away, True).wait_send()
        sq_copy(away, False).wait_recv()
    squares[pl.ds(1 + me, 1)] = squares[0:1]
    everyone = squares[1]
    for q in range(1, n):
        everyone += squares[1 + q]
    squares_ref[...] = everyone
    for pair in range(chunks // 2):
        full_copy(pair).wait()
    for g in range(chunks, groups):
        own_copy(g).wait()


def gradients_of(n, x, dy, wg, wu, wd):
    _, tokens, d = x.shape
    _, ff, _ = wd.shape
    chunks, hops = ff // CHUNK, n // 2
    shard_rows = 3 * d // n
    v, dma = pltpu.VMEM, pltpu.SemaphoreType.DMA
    anyspace = pl.BlockSpec(memory_space=pl.ANY)
    return pl.pallas_call(
        functools.partial(gradients_body, n),
        out_shape=(
            jax.ShapeDtypeStruct((chunks, n * shard_rows, CHUNK), BF16),
            jax.ShapeDtypeStruct((chunks, shard_rows, CHUNK), BF16),
            jax.ShapeDtypeStruct((8, CHUNK), F32),
        ),
        in_specs=[anyspace] * 5,
        out_specs=(anyspace, anyspace, pl.BlockSpec(memory_space=pltpu.VMEM)),
        scratch_shapes=[
            v((tokens, d), BF16), v((d, tokens), BF16), v((tokens, d), BF16), v((d, tokens), BF16),
            v((tokens, d), BF16), v((tokens, d), BF16), v((tokens, d), F32),
            v((d, ff), BF16), v((d, ff), BF16), v((ff, d), BF16),
            v((2, d, 2 * CHUNK), BF16), v((2, CHUNK, d), BF16),
            v((2, TILE, CHUNK), BF16), v((2, TILE, 2 * CHUNK), BF16),
            v((CHUNK, d), F32), v((d, 2 * CHUNK), F32),
            v((2 * chunks, n * shard_rows, CHUNK), BF16),
            v((2, hops, 2, shard_rows, CHUNK), BF16), v((2, hops - 1, 2, shard_rows, CHUNK), BF16),
            v((n + 1, 8, CHUNK), F32),
            dma((5,)), dma((2, 3)), dma((2, hops, 2)), dma((2, hops, 2)), dma((2, hops, 2)), dma((2, hops, 2)),
            dma((n - 1,)), dma((n,)), dma((chunks // 2,)), dma((chunks,)),
        ],
        compiler_params=pltpu.CompilerParams(vmem_limit_bytes=VMEM_LIMIT, collective_id=0, has_side_effects=True),
        name="gradients",
    )(x, dy, wg, wu, wd)


def adamw_body(n, factor_ref, g_ref, *refs):
    wmv, new = refs[:9], refs[-9:]
    factor = factor_ref[0]
    rows_g = g_ref.shape[1] // n
    d = wmv[0].shape[1]
    rd, rf = d // n, CHUNK // n

    def update(i, r, c, g):
        g = g.astype(F32) * factor
        w, m, v = (wmv[3 * k + i][0, r, c].astype(F32) for k in range(3))
        m = 0.9 * m + 0.1 * g
        v = 0.95 * v + 0.05 * g * g
        w = w - 0.02 * (m * lax.rsqrt(v + 1e-8) + 0.1 * w)
        for k, value in enumerate((w, m, v)):
            new[3 * k + i][0, r, c] = value.astype(new[3 * k + i].dtype)

    for r in range(n):
        at = r * rows_g
        for i in range(2):
            update(i, slice(r * rd, (r + 1) * rd), slice(None), g_ref[0, at + i * rd : at + (i + 1) * rd, :])
        for q in range(d // CHUNK):
            update(2, slice(r * rf, (r + 1) * rf), slice(q * CHUNK, (q + 1) * CHUNK), g_ref[0, at + 2 * rd + q * rf : at + 2 * rd + (q + 1) * rf, :])


def adamw(n, layer, factor, g, wmv, before):
    layers, d, ff = wmv[0].shape
    wide = pl.BlockSpec((1, d, CHUNK), lambda c: (layer, 0, c))
    tall = pl.BlockSpec((1, CHUNK, d), lambda c: (layer, c, 0))
    nine = [wide, wide, tall] * 3
    count = layers * d * ff
    return pl.pallas_call(
        functools.partial(adamw_body, n),
        grid=(ff // CHUNK,),
        out_shape=[jax.ShapeDtypeStruct(a.shape, a.dtype) for a in wmv],
        in_specs=[pl.BlockSpec(memory_space=pltpu.SMEM), pl.BlockSpec((1, g.shape[1], CHUNK), lambda c: (c, 0, 0)), *nine]
        + [pl.BlockSpec(memory_space=pl.ANY)] * len(before),
        out_specs=nine,
        input_output_aliases={11 + i: i for i in range(len(before))},
        compiler_params=pltpu.CompilerParams(vmem_limit_bytes=VMEM_LIMIT, dimension_semantics=("arbitrary",)),
        cost_estimate=pl.CostEstimate(flops=60 * count, bytes_accessed=33 * count, transcendentals=3 * count),
        name=f"adamw{layer}",
    )(factor, g, *wmv, *before)


def gathered(n, own):
    hops = n // 2
    half = own.shape[1] // 2
    right = [(i, (i + 1) % n) for i in range(n)]
    left = [(i, (i - 1) % n) for i in range(n)]
    me = lax.axis_index(AXIS)
    parts = {0: own}
    a = b = own
    for j in range(1, hops):
        a, b = lax.ppermute(a, AXIS, right), lax.ppermute(b, AXIS, left)
        parts[-j], parts[j] = a, b
    a, b = lax.ppermute(a[:, :half], AXIS, right), lax.ppermute(b[:, half:], AXIS, left)
    parts[hops] = jnp.concatenate([a, b], axis=1)
    by_away = jnp.stack([parts[j] for j in range(1 - hops, hops + 1)])
    return jnp.roll(by_away, me + 1 - hops, axis=0).transpose(1, 0, 2, 3).reshape(own.shape[0], -1, own.shape[2])


def solution(mesh):
    n = mesh.shape[AXIS]

    def step(x, dy, *wmv):
        full, own, squares = gradients_of(n, x, dy, *wmv[:3])
        count = sum(w.size for w in wmv[:3])
        factor = jnp.minimum(1.0, 0.5 * lax.rsqrt(jnp.sum(squares) / count + 1e-30)).reshape(1)
        new = adamw(n, 1, factor, full, wmv, ())
        new = adamw(n, 0, factor, gathered(n, own), wmv, new)
        return tuple(new)

    return jax.shard_map(
        step,
        mesh=mesh,
        in_specs=(P(("rep", "dp"), None, None),) * 2 + (P(None, None, None),) * 9,
        out_specs=(P("rep", None, None),) * 9,
        check_vma=False,
    )
```

```python
import functools

import jax
import jax.numpy as jnp
from jax import lax
from jax.experimental import pallas as pl
from jax.experimental.pallas import tpu as pltpu
from jax.sharding import PartitionSpec as P

F32, BF16 = jnp.float32, jnp.bfloat16
AXIS = "dp"
FTILE = 512
TILE = 1024
CHUNK = 256
VMEM_LIMIT = 67043328
ADAMW_VMEM = VMEM_LIMIT


def mm(a, b):
    return jnp.dot(a, b, preferred_element_type=F32)


def mm_nt(a, b):
    return lax.dot_general(a, b, (((1,), (1,)), ((), ())), preferred_element_type=F32)


def mm_tn(a, b):
    return lax.dot_general(a, b, (((0,), (0,)), ((), ())), preferred_element_type=F32)


def sigmoid(x):
    return 0.5 * jnp.tanh(0.5 * x) + 0.5


def normed(wide):
    scale = lax.rsqrt(jnp.mean(wide * wide, -1, keepdims=True) + 1e-6)
    return (wide * scale).astype(BF16)


def gradients_body(n, x_hbm, dy_hbm, wg_hbm, wu_hbm, wd_hbm, full_hbm, own_hbm, squares_ref,
                   a0, a0t, a1, a1t, dy, h1, acc, w0g, w0u, w0d, w1, w1d, act, dgu, accd, accgu, grads, slots, sums, squares,
                   first_sem, w1_sem, rs_send, rs_recv, ag_send, ag_recv, sq_send, sq_recv, full_sem, own_sem):
    tokens, d = h1.shape
    ff = w0d.shape[0]
    tiles, chunks = tokens // TILE, ff // CHUNK
    groups = 2 * chunks
    hops = n // 2
    shard_rows = grads.shape[1] // n
    half = shard_rows // 2
    me = lax.axis_index(AXIS)
    to = (lax.rem(me + 1, n), lax.rem(me + n - 1, n))

    def rows(t):
        return pl.ds(pl.multiple_of(t * TILE, TILE), TILE)

    def frows(t):
        return pl.ds(pl.multiple_of(t * FTILE, FTILE), FTILE)

    def cols(c):
        return pl.ds(pl.multiple_of(c * CHUNK, CHUNK), CHUNK)

    def shard(away):
        return pl.multiple_of(lax.rem(me + away + n, n) * shard_rows, shard_rows)

    def remote(src, dst, send, recv, way):
        return pltpu.make_async_remote_copy(src_ref=src, dst_ref=dst, send_sem=send, recv_sem=recv, device_id={AXIS: to[way]}, device_id_type=pl.DeviceIdType.MESH)

    def rs_copy(s, g, way):
        p = lax.rem(g, 2)
        if s == 1:
            part = pl.ds(way * half, half)
            src, dst = grads.at[g, pl.ds(shard(hops) + way * half, half)], slots.at[way, 0, p, part]
        else:
            src, dst = sums.at[way, s - 2, p], slots.at[way, s - 1, p]
        return remote(src, dst, rs_send.at[way, s - 1, p], rs_recv.at[way, s - 1, p], way)

    def rs_add(s, g):
        p = lax.rem(g, 2)
        for way in range(2):
            own = grads[g, pl.ds(shard((1 - 2 * way) * (hops + 1 - s)), shard_rows)]
            if s == 2:
                here = slice(way * half, way * half + half)
                there = slice(half - way * half, shard_rows - way * half)
                sums[way, 0, p, there] = own[there]
                sums[way, 0, p, here] = (slots[way, 0, p, here].astype(F32) + own[here].astype(F32)).astype(BF16)
            else:
                sums[way, s - 2, p] = (slots[way, s - 2, p].astype(F32) + own.astype(F32)).astype(BF16)

    def rs_final(g):
        p = lax.rem(g, 2)
        mine = pl.ds(shard(0), shard_rows)
        total = slots[0, hops - 1, p].astype(F32) + slots[1, hops - 1, p].astype(F32) + grads[g, mine].astype(F32)
        total = total.astype(BF16)
        grads[g, mine] = total
        wide = total.astype(F32)
        squares[0] += jnp.sum((wide * wide).reshape(shard_rows // 8, 8, CHUNK), axis=0)

    def ag_copies(pair, j, whole):
        copies = []
        for b in range(2):
            for way in range(2):
                at = shard((2 * way - 1) * j)
                part = pl.ds(at, shard_rows) if whole else pl.ds(at + way * half, half)
                ref = grads.at[2 * pair + b, part]
                copies.append(remote(ref, ref, ag_send.at[way, j, b, lax.rem(pair, 2)], ag_recv.at[way, j, b, lax.rem(pair, 2)], way))
        return copies

    def full_copy(pair):
        return pltpu.make_async_copy(grads.at[pl.ds(2 * pair, 2)], full_hbm.at[pl.ds(2 * pair, 2)], full_sem.at[pair])

    def own_copy(g):
        return pltpu.make_async_copy(grads.at[g, pl.ds(shard(0), shard_rows)], own_hbm.at[g - chunks], own_sem.at[g - chunks])

    pairs = chunks // 2

    def tick(t):
        def group(g, f):
            pl.when((g >= 0) & (g < groups))(functools.partial(f, g))

        def arrived(s, g):
            for way in range(2):
                rs_copy(s, g, way).wait()

        def add(s, g):
            arrived(s - 1, g)
            rs_add(s, g)

        def final(g):
            arrived(hops, g)
            rs_final(g)

        def send(s, g):
            for way in range(2):
                rs_copy(s, g, way).start()

        for s in range(hops, 1, -1):
            group(t - s, functools.partial(add, s))
        group(t - hops - 1, final)
        for s in range(hops, 0, -1):
            group(t - s, functools.partial(send, s))

        e = lax.rem(t + hops, 2)
        u = (t - hops - 2 - 3 * e) // 2

        def gathering(u, f):
            pair, j = 2 * (u // hops) + e, lax.rem(u + 2 * hops, hops)
            for whole in (True, False):
                pl.when((u >= 0) & (pair < pairs) & ((j < hops - 1) == whole))(functools.partial(f, pair, j, whole))

        def landed(pair, j, whole):
            for copy in ag_copies(pair, j, whole):
                copy.wait()
            if not whole:
                full_copy(pair).start()

        def pass_on(pair, j, whole):
            for copy in ag_copies(pair, j, whole):
                copy.start()

        gathering(u - 1, landed)
        gathering(u, pass_on)

        g = t - hops - 2

        @pl.when((g >= chunks) & (g < groups))
        def _():
            own_copy(g).start()

    def w1_copies(c):
        slot = lax.rem(c, 2)
        return (
            pltpu.make_async_copy(wg_hbm.at[1, :, cols(c)], w1.at[slot, :, pl.ds(0, CHUNK)], w1_sem.at[slot, 0]),
            pltpu.make_async_copy(wu_hbm.at[1, :, cols(c)], w1.at[slot, :, pl.ds(CHUNK, CHUNK)], w1_sem.at[slot, 1]),
            pltpu.make_async_copy(wd_hbm.at[1, cols(c), :], w1d.at[slot], w1_sem.at[slot, 2]),
        )

    squares[...] = jnp.zeros_like(squares)
    barrier = pltpu.get_barrier_semaphore()
    for away in range(1, n):
        pl.semaphore_signal(barrier, inc=1, device_id={AXIS: lax.rem(me + away, n)}, device_id_type=pl.DeviceIdType.MESH)

    first = (
        pltpu.make_async_copy(x_hbm.at[0], h1, first_sem.at[0]),
        pltpu.make_async_copy(wg_hbm.at[0], w0g, first_sem.at[1]),
        pltpu.make_async_copy(wu_hbm.at[0], w0u, first_sem.at[2]),
        pltpu.make_async_copy(wd_hbm.at[0], w0d, first_sem.at[3]),
        pltpu.make_async_copy(dy_hbm.at[0], dy, first_sem.at[4]),
    )
    for copy in first + w1_copies(0) + w1_copies(1):
        copy.start()

    def norm0(t):
        a = normed(h1[frows(t), :].astype(F32))
        a0[frows(t), :] = a
        a0t[:, frows(t)] = a.T

    def expand(t):
        a = a0[frows(t), :]
        b = lax.rem(t, 2) * chunks
        for c in range(chunks):
            s = pl.ds(c * CHUNK, CHUNK)
            gate, up = mm(a, w0g[:, s]), mm(a, w0u[:, s])
            grads[b + c, :FTILE, :] = (gate * sigmoid(gate) * up).astype(BF16)

    def contract(t):
        b = lax.rem(t, 2) * chunks
        out = mm(grads[b, :FTILE, :], w0d[:CHUNK, :])
        for c in range(1, chunks):
            out += mm(grads[b + c, :FTILE, :], w0d[c * CHUNK : (c + 1) * CHUNK, :])
        h = (h1[frows(t), :].astype(F32) + out.astype(BF16).astype(F32)).astype(BF16)
        h1[frows(t), :] = h
        a = normed(h.astype(F32))
        a1[frows(t), :] = a
        a1t[:, frows(t)] = a.T
        acc[frows(t), :] = jnp.zeros((FTILE, d), F32)

    first[0].wait()
    norm0(0)
    norm0(1)
    accd[...] = jnp.zeros_like(accd)
    accgu[...] = jnp.zeros_like(accgu)
    first[1].wait()
    first[2].wait()
    expand(0)
    first[3].wait()

    ftiles = tokens // FTILE

    def forward(t, _):
        contract(t)
        expand(t + 1)
        norm0(jnp.minimum(t + 2, ftiles - 1))
        return 0

    lax.fori_loop(0, ftiles - 1, forward, 0)
    contract(ftiles - 1)
    first[4].wait()
    pl.semaphore_wait(barrier, n - 1)

    def elementwise(gate, up, dact):
        s = sigmoid(gate)
        p = gate * s
        act[...] = (p * up).astype(BF16)
        dact = dact.astype(BF16).astype(F32)
        dgu[:, CHUNK:] = (dact * p).astype(BF16)
        dgu[:, :CHUNK] = (dact * up * (s + p * (1.0 - s))).astype(BF16)

    def finish(g):
        rd, rf = d // n, CHUNK // n
        for r in range(n):
            at = r * shard_rows
            grads[g, at : at + rd, :] = accgu[r * rd : (r + 1) * rd, :CHUNK].astype(BF16)
            grads[g, at + rd : at + 2 * rd, :] = accgu[r * rd : (r + 1) * rd, CHUNK:].astype(BF16)
            for q in range(d // CHUNK):
                grads[g, at + 2 * rd + q * rf : at + 2 * rd + (q + 1) * rf, :] = accd[r * rf : (r + 1) * rf, q * CHUNK : (q + 1) * CHUNK].astype(BF16)
        accd[...] = jnp.zeros_like(accd)
        accgu[...] = jnp.zeros_like(accgu)

    total = chunks * tiles

    def front1(i):
        c, t = i // tiles, lax.rem(i, tiles)
        slot = lax.rem(c, 2)
        a = a1[rows(t), :]
        elementwise(mm(a, w1[slot, :, :CHUNK]), mm(a, w1[slot, :, CHUNK:]), mm_nt(dy[rows(t), :], w1d[slot]))

    def back1(i):
        c, t = i // tiles, lax.rem(i, tiles)
        accgu[...] += mm(a1t[:, rows(t)], dgu[...])
        accd[...] += mm_tn(act[...], dy[rows(t), :])
        acc[rows(t), :] += mm_nt(dgu[...], w1[lax.rem(c, 2)])

    def layer1(i, _):
        c, t = i // tiles, lax.rem(i, tiles)

        @pl.when((t == tiles - 1) & (c + 1 < chunks))
        def _():
            for copy in w1_copies(c + 1):
                copy.wait()

        back1(i)
        front1(jnp.minimum(i + 1, total - 1))

        @pl.when(t == tiles - 1)
        def _():
            finish(c)

            @pl.when(c + 2 < chunks)
            def _():
                for copy in w1_copies(c + 2):
                    copy.start()

            tick(c + 1)

        return 0

    for copy in w1_copies(0):
        copy.wait()
    front1(0)
    lax.fori_loop(0, total, layer1, 0)

    def between(t, _):
        da = acc[rows(t), :].astype(BF16).astype(F32)
        wide = h1[rows(t), :].astype(F32)
        scale = lax.rsqrt(jnp.mean(wide * wide, -1, keepdims=True) + 1e-6)
        along = jnp.sum(da * wide, -1, keepdims=True) * (scale * scale * scale / d)
        through = (da * scale - wide * along).astype(BF16).astype(F32)
        dy[rows(t), :] = (dy[rows(t), :].astype(F32) + through).astype(BF16)
        return 0

    lax.fori_loop(0, tiles, between, 0)

    def front0(i):
        c, t = i // tiles, lax.rem(i, tiles)
        a = a0[rows(t), :]
        elementwise(mm(a, w0g[:, cols(c)]), mm(a, w0u[:, cols(c)]), mm_nt(dy[rows(t), :], w0d[cols(c), :]))

    def layer0(i, _):
        c, t = i // tiles, lax.rem(i, tiles)
        accgu[...] += mm(a0t[:, rows(t)], dgu[...])
        accd[...] += mm_tn(act[...], dy[rows(t), :])
        front0(jnp.minimum(i + 1, total - 1))

        @pl.when(t == tiles - 1)
        def _():
            finish(chunks + c)
            tick(chunks + c + 1)

        return 0

    front0(0)
    lax.fori_loop(0, total, layer0, 0)

    def sq_copy(away, mine):
        q = me if mine else lax.rem(me + away, n)
        return pltpu.make_async_remote_copy(
            src_ref=squares.at[0], dst_ref=squares.at[1 + q], send_sem=sq_send.at[away - 1], recv_sem=sq_recv.at[q],
            device_id={AXIS: lax.rem(me + away, n)}, device_id_type=pl.DeviceIdType.MESH)

    last = max(groups + hops + 1, *(hops + 2 + 3 * e + 2 * hops * ((pairs + 1 - e) // 2) for e in range(2)))

    def drain(t, _):
        tick(t)

        @pl.when(t == groups + hops)
        def _():
            for away in range(1, n):
                sq_copy(away, True).start()

        return 0

    lax.fori_loop(groups + 1, last + 1, drain, 0)
    for away in range(1, n):
        sq_copy(away, True).wait_send()
        sq_copy(away, False).wait_recv()
    squares[pl.ds(1 + me, 1)] = squares[0:1]
    everyone = squares[1]
    for q in range(1, n):
        everyone += squares[1 + q]
    squares_ref[...] = everyone
    for pair in range(chunks // 2):
        full_copy(pair).wait()
    for g in range(chunks, groups):
        own_copy(g).wait()


def gradients_of(n, x, dy, wg, wu, wd):
    _, tokens, d = x.shape
    _, ff, _ = wd.shape
    chunks, hops = ff // CHUNK, n // 2
    shard_rows = 3 * d // n
    v, dma = pltpu.VMEM, pltpu.SemaphoreType.DMA
    anyspace = pl.BlockSpec(memory_space=pl.ANY)
    return pl.pallas_call(
        functools.partial(gradients_body, n),
        out_shape=(
            jax.ShapeDtypeStruct((chunks, n * shard_rows, CHUNK), BF16),
            jax.ShapeDtypeStruct((chunks, shard_rows, CHUNK), BF16),
            jax.ShapeDtypeStruct((8, CHUNK), F32),
        ),
        in_specs=[anyspace] * 5,
        out_specs=(anyspace, anyspace, pl.BlockSpec(memory_space=pltpu.VMEM)),
        scratch_shapes=[
            v((tokens, d), BF16), v((d, tokens), BF16), v((tokens, d), BF16), v((d, tokens), BF16),
            v((tokens, d), BF16), v((tokens, d), BF16), v((tokens, d), F32),
            v((d, ff), BF16), v((d, ff), BF16), v((ff, d), BF16),
            v((2, d, 2 * CHUNK), BF16), v((2, CHUNK, d), BF16),
            v((TILE, CHUNK), BF16), v((TILE, 2 * CHUNK), BF16),
            v((CHUNK, d), F32), v((d, 2 * CHUNK), F32),
            v((2 * chunks, n * shard_rows, CHUNK), BF16),
            v((2, hops, 2, shard_rows, CHUNK), BF16), v((2, hops - 1, 2, shard_rows, CHUNK), BF16),
            v((n + 1, 8, CHUNK), F32),
            dma((5,)), dma((2, 3)), dma((2, hops, 2)), dma((2, hops, 2)), dma((2, hops, 2, 2)), dma((2, hops, 2, 2)),
            dma((n - 1,)), dma((n,)), dma((chunks // 2,)), dma((chunks,)),
        ],
        compiler_params=pltpu.CompilerParams(vmem_limit_bytes=VMEM_LIMIT, collective_id=0, has_side_effects=True),
        name="gradients",
    )(x, dy, wg, wu, wd)


def adamw_update(factor, wmv, new, i, at, g):
    g = g.astype(F32) * factor
    w, m, v = (wmv[3 * k + i][at].astype(F32) for k in range(3))
    m = 0.9 * m + 0.1 * g
    v = 0.95 * v + 0.05 * g * g
    w = w - 0.02 * (m * lax.rsqrt(v + 1e-8) + 0.1 * w)
    for k, value in enumerate((w, m, v)):
        new[3 * k + i][at] = value.astype(new[3 * k + i].dtype)


def adamw_whole_body(n, factor_ref, g_ref, *refs):
    wmv, new = refs[:9], refs[-9:]
    rows_g = g_ref.shape[1] // n
    d = wmv[0].shape[1]
    rd, rf = d // n, CHUNK // n
    update = functools.partial(adamw_update, factor_ref[0], wmv, new)
    for r in range(n):
        at = r * rows_g
        for i in range(2):
            update(i, (0, slice(r * rd, (r + 1) * rd)), g_ref[0, at + i * rd : at + (i + 1) * rd, :])
        for q in range(d // CHUNK):
            update(2, (0, 0, slice(r * rf, (r + 1) * rf), slice(q * CHUNK, (q + 1) * CHUNK)), g_ref[0, at + 2 * rd + q * rf : at + 2 * rd + (q + 1) * rf, :])


def adamw_shards_body(arrays, rs_ref, factor_ref, *refs):
    gs, wmv, new = refs[:arrays], refs[arrays : arrays + 9], refs[-9:]
    rd, rf = wmv[0].shape[1], wmv[2].shape[2]
    d = wmv[2].shape[3]
    update = functools.partial(adamw_update, factor_ref[0], wmv, new)
    for k, g_ref in enumerate(gs):

        @pl.when(pl.program_id(0) == k)
        def _():
            for c in range(g_ref.shape[0]):
                for i in range(2):
                    update(i, (0, slice(None), slice(c * CHUNK, (c + 1) * CHUNK)), g_ref[c, i * rd : (i + 1) * rd, :])
                for q in range(d // CHUNK):
                    update(2, (0, c, slice(None), slice(q * CHUNK, (q + 1) * CHUNK)), g_ref[c, 2 * rd + q * rf : 2 * rd + (q + 1) * rf, :])


def adamw_call(name, body, grid, prefetch, gs, g_specs, blocks, wmv, before, part):
    count = int(sum(w.size for w in wmv[:3]) * part)
    first = len(prefetch) + 1 + len(gs) + 9
    return pl.pallas_call(
        body,
        grid_spec=pltpu.PrefetchScalarGridSpec(
            num_scalar_prefetch=len(prefetch) - 1,
            grid=grid,
            in_specs=[pl.BlockSpec(memory_space=pltpu.SMEM), *g_specs, *blocks, *[pl.BlockSpec(memory_space=pl.ANY)] * len(before)],
            out_specs=blocks,
        ),
        out_shape=[jax.ShapeDtypeStruct(a.shape, a.dtype) for a in wmv],
        input_output_aliases={first - 1 + i: i for i in range(len(before))},
        compiler_params=pltpu.CompilerParams(vmem_limit_bytes=ADAMW_VMEM, dimension_semantics=("arbitrary",) * len(grid)),
        cost_estimate=pl.CostEstimate(flops=400 * count, bytes_accessed=22 * count, transcendentals=count),
        name=name,
    )(*prefetch, *gs, *wmv, *before)


def adamw_whole(n, layer, chunks, factor, g, wmv, before):
    lo, hi = chunks
    _, d, ff = wmv[0].shape
    wide = pl.BlockSpec((1, d, CHUNK), lambda c: (layer, 0, c + lo))
    tall = pl.BlockSpec((1, 1, CHUNK, d), lambda c: (layer, c + lo, 0, 0))
    g_spec = pl.BlockSpec((1, g.shape[1], CHUNK), lambda c: (c + lo, 0, 0))
    part = (hi - lo) * CHUNK / (ff * wmv[0].shape[0])
    return adamw_call(f"adamw_{layer}_{lo}", functools.partial(adamw_whole_body, n), (hi - lo,), (factor,), (g,), [g_spec], [wide, wide, tall] * 3, wmv, before, part)


def adamw_shards(n, layer, parts, steps, factor, wmv, before):
    layers, d, ff = wmv[0].shape
    chunks = ff // CHUNK
    each = parts[0][2].shape[0] // steps
    start = parts[1][1] - parts[0][1] if len(parts) > 1 else 0

    def block(k, c):
        return c + k * (start // each)

    rs = jnp.stack([r for r, _, _ in parts]).astype(jnp.int32)
    wide = pl.BlockSpec((1, d // n, each * CHUNK), lambda k, c, rs: (layer, rs[k], block(k, c)))
    tall = pl.BlockSpec((1, each, CHUNK // n, d), lambda k, c, rs: (layer, block(k, c), rs[k], 0))
    shape = (each, *parts[0][2].shape[1:])
    g_specs = [pl.BlockSpec(shape, lambda k, c, rs, i=i: (jnp.where(k == i, c, jnp.where(k < i, 0, steps - 1)), 0, 0)) for i in range(len(parts))]
    part = sum(g.shape[0] for _, _, g in parts) / (chunks * n * layers)
    return adamw_call(f"adamw_{layer}_of_{len(parts)}", functools.partial(adamw_shards_body, len(parts)), (len(parts), steps), (rs, factor), [g for _, _, g in parts], g_specs, [wide, wide, tall] * 3, wmv, before, part)


def solution(mesh):
    n = mesh.shape[AXIS]
    hops = n // 2
    right = [(i, (i + 1) % n) for i in range(n)]
    left = [(i, (i - 1) % n) for i in range(n)]

    def step(x, dy, *wmv):
        full, own, squares = gradients_of(n, x, dy, *wmv[:3])
        layers, d, ff = wmv[0].shape
        chunks = ff // CHUNK
        count = sum(w.size for w in wmv[:3])
        factor = jnp.minimum(1.0, 0.5 * lax.rsqrt(jnp.sum(squares) / count + 1e-30)).reshape(1)
        wmv = [a.reshape(layers, chunks, CHUNK, d) if i % 3 == 2 else a for i, a in enumerate(wmv)]
        me = lax.axis_index(AXIS)

        def of(away):
            return lax.rem(me + away + n, n)

        a, b = lax.ppermute(own, AXIS, right), lax.ppermute(own, AXIS, left)
        most = chunks - 2
        new = adamw_whole(n, 1, (0, most), factor, full, wmv, ())
        a, b, *new = lax.optimization_barrier((a, b, *new))
        here = [(of(0), 0, own), (of(-1), 0, a), (of(1), 0, b)]
        for j in range(1, hops):
            if j < hops - 1:
                a2, b2 = lax.ppermute(a, AXIS, right), lax.ppermute(b, AXIS, left)
            else:
                a2, b2 = lax.ppermute(a[: chunks // 2], AXIS, right), lax.ppermute(b[chunks // 2 :], AXIS, left)
            if j == 1:
                new = adamw_whole(n, 1, (most, chunks), factor, full, wmv, new)
            new = adamw_shards(n, 0, here, 4, factor, wmv, new)
            a, b, *new = lax.optimization_barrier((a2, b2, *new))
            here = [(of(-1 - j), 0, a), (of(1 + j), 0, b)]
        new = adamw_shards(n, 0, [(of(hops), 0, a), (of(hops), chunks // 2, b)], 2, factor, wmv, new)
        return tuple(new_one.reshape(layers, ff, d) if i % 3 == 2 else new_one for i, new_one in enumerate(new))

    return jax.shard_map(
        step,
        mesh=mesh,
        in_specs=(P(("rep", "dp"), None, None),) * 2 + (P(None, None, None),) * 9,
        out_specs=(P("rep", None, None),) * 9,
        check_vma=False,
    )
```

```python
import functools

import jax
import jax.numpy as jnp
from jax import lax
from jax.experimental import pallas as pl
from jax.experimental.pallas import tpu as pltpu
from jax.sharding import PartitionSpec as P

F32, BF16 = jnp.float32, jnp.bfloat16
AXIS = "dp"
FTILE = 512
TILE = 1024
SPACING = 3
RING = 5
AG_SPACING = 6
CHUNK = 256
VMEM_LIMIT = 67043328
STEPS = 2


def mm(a, b):
    return jnp.dot(a, b, preferred_element_type=F32)


def mm_nt(a, b):
    return lax.dot_general(a, b, (((1,), (1,)), ((), ())), preferred_element_type=F32)


def mm_tn(a, b):
    return lax.dot_general(a, b, (((0,), (0,)), ((), ())), preferred_element_type=F32)


def sigmoid(x):
    return 0.5 * jnp.tanh(0.5 * x) + 0.5


def normed(wide):
    scale = lax.rsqrt(jnp.mean(wide * wide, -1, keepdims=True) + 1e-6)
    return (wide * scale).astype(BF16)


def gradients_body(n, x_hbm, dy_hbm, wg_hbm, wu_hbm, wd_hbm, full_hbm, own_lo_hbm, own_hi_hbm, factor_ref, me_ref, kept_hbm,
                   a0, a0t, a1, a1t, dy, h1, w0g, w0u, w0d, w1, w1d, act, dgu, piece, accd, accgu, grads, slots, sums, squares,
                   first_sem, w1_sem, w1d_sem, rs_send, rs_recv, ag_send, ag_recv, sq_send, sq_recv, full_sem, own_sem, keep_sem, piece_sem):
    tokens, d = h1.shape
    ff = w0d.shape[0]
    tiles, chunks = tokens // TILE, ff // CHUNK
    groups = 2 * chunks
    hops = n // 2
    shard_rows = grads.shape[1] // n
    half = shard_rows // 2
    me = lax.axis_index(AXIS)
    own_hbm = (own_lo_hbm, own_hi_hbm)
    to = (lax.rem(me + 1, n), lax.rem(me + n - 1, n))

    def rows(t):
        return pl.ds(pl.multiple_of(t * TILE, TILE), TILE)

    def frows(t):
        return pl.ds(pl.multiple_of(t * FTILE, FTILE), FTILE)

    def cols(c):
        return pl.ds(pl.multiple_of(c * CHUNK, CHUNK), CHUNK)

    def shard(away):
        return pl.multiple_of(lax.rem(me + away + n, n) * shard_rows, shard_rows)

    def place(g):
        return jnp.where(g < chunks, g, chunks + lax.rem(g - chunks + RING, RING))

    def remote(src, dst, send, recv, way):
        return pltpu.make_async_remote_copy(src_ref=src, dst_ref=dst, send_sem=send, recv_sem=recv, device_id={AXIS: to[way]}, device_id_type=pl.DeviceIdType.MESH)

    def rs_copy(s, g, way):
        p = lax.rem(g, 2)
        if s == 1:
            part = pl.ds(way * half, half)
            src, dst = grads.at[place(g), pl.ds(shard(hops) + way * half, half)], slots.at[way, 0, p, part]
        else:
            src, dst = sums.at[way, s - 2], slots.at[way, s - 1, p]
        return remote(src, dst, rs_send.at[way, s - 1, p], rs_recv.at[way, s - 1, p], way)

    def rs_add(s, g):
        p = lax.rem(g, 2)
        for way in range(2):
            own = grads[place(g), pl.ds(shard((1 - 2 * way) * (hops + 1 - s)), shard_rows)]
            if s == 2:
                here = slice(way * half, way * half + half)
                there = slice(half - way * half, shard_rows - way * half)
                sums[way, 0, there] = own[there]
                sums[way, 0, here] = (slots[way, 0, p, here].astype(F32) + own[here].astype(F32)).astype(BF16)
            else:
                sums[way, s - 2] = (slots[way, s - 2, p].astype(F32) + own.astype(F32)).astype(BF16)

    def rs_final(g):
        p = lax.rem(g, 2)
        mine = pl.ds(shard(0), shard_rows)
        total = slots[0, hops - 1, p].astype(F32) + slots[1, hops - 1, p].astype(F32) + grads[place(g), mine].astype(F32)
        total = total.astype(BF16)
        grads[place(g), mine] = total
        wide = total.astype(F32)
        squares[0] += jnp.sum((wide * wide).reshape(shard_rows // 8, 8, CHUNK), axis=0)

    def ag_copies(pair, j, whole):
        copies = []
        for b in range(2):
            for way in range(2):
                at = shard((2 * way - 1) * j)
                part = pl.ds(at, shard_rows) if whole else pl.ds(at + way * half, half)
                ref = grads.at[2 * pair + b, part]
                copies.append(remote(ref, ref, ag_send.at[way, j, b, lax.rem(pair, 2)], ag_recv.at[way, j, b, lax.rem(pair, 2)], way))
        return copies

    def full_copy(pair):
        return pltpu.make_async_copy(grads.at[pl.ds(2 * pair, 2)], full_hbm.at[pl.ds(2 * pair, 2)], full_sem.at[pair])

    def own_copy(g, part):
        return pltpu.make_async_copy(grads.at[place(g), pl.ds(shard(0), shard_rows)], own_hbm[part].at[g - chunks - part * (chunks // 2)], own_sem.at[g - chunks])

    def own_copies(g, f):
        for part in range(2):
            lo = chunks + part * (chunks // 2)

            @pl.when((g >= lo) & (g < lo + chunks // 2))
            def _():
                f(own_copy(g, part))

    pairs = chunks // 2

    total, ftiles = chunks * tiles, tokens // FTILE
    later = total + ftiles
    over = later + total

    ag_lag = -((2 - hops * SPACING) // tiles) + 1
    in_layer0 = (total - 2) // AG_SPACING + 1

    def tick(i):
        def group(s, f):
            step = i - (s - 1) * SPACING - (tiles - 1)
            last_layer = (step >= 0) & (step < total)
            first_layer = (step >= later) & (step < over)
            step = jnp.where(first_layer, step - ftiles, step)
            pl.when((last_layer | first_layer) & (lax.rem(step + tiles * groups, tiles) == 0))(functools.partial(f, step // tiles))

        def hop(s, g):
            if s > 1:
                for way in range(2):
                    rs_copy(s - 1, g, way).wait()
                rs_add(s, g)
            for way in range(2):
                rs_copy(s, g, way).start()

        def final(g):
            for way in range(2):
                rs_copy(hops, g, way).wait()
            rs_final(g)
            own_copies(g - 1, lambda copy: copy.wait())
            own_copies(g, lambda copy: copy.start())

        group(hops + 1, final)
        for s in range(hops, 0, -1):
            group(s, functools.partial(hop, s))

        chance = jnp.where(
            i < total, i // tiles - 1, jnp.where(
                i < later, chunks - 1 + (i - total) // 2, jnp.where(
                    i < over, chunks - 1 + ftiles // 2 + (i - later) // AG_SPACING, chunks - 1 + ftiles // 2 + in_layer0 + (i - over) // 2)))
        due = jnp.where(
            i < total, lax.rem(i, tiles) == 1, jnp.where(
                i < later, lax.rem(i - total, 2) == 1, jnp.where(
                    i < over, lax.rem(i - later, AG_SPACING) == 1, lax.rem(i - over, 2) == 1)))
        chance = chance - ag_lag

        @pl.when(due & (chance >= 0))
        def _():
            e = lax.rem(chance + 2 * groups, 2)
            u = (chance - 3 * e) // 2

            def gathering(u, f):
                pair, j = 2 * (u // hops) + e, lax.rem(u + 2 * hops, hops)
                for whole in (True, False):
                    pl.when((chance >= 3 * e) & (u >= 0) & (pair < pairs) & ((j < hops - 1) == whole))(functools.partial(f, pair, j, whole))

            def landed(pair, j, whole):
                for copy in ag_copies(pair, j, whole):
                    copy.wait()
                if not whole:
                    full_copy(pair).start()

            def pass_on(pair, j, whole):
                for copy in ag_copies(pair, j, whole):
                    copy.start()

            gathering(u - 1, landed)
            gathering(u, pass_on)

    def both(c):
        return pl.ds(pl.multiple_of(c * 2 * CHUNK, 2 * CHUNK), 2 * CHUNK)

    def w1_copies(c):
        return (
            pltpu.make_async_copy(wg_hbm.at[1, :, cols(c)], w1.at[:, pl.ds(c * 2 * CHUNK, CHUNK)], w1_sem.at[c, 0]),
            pltpu.make_async_copy(wu_hbm.at[1, :, cols(c)], w1.at[:, pl.ds(c * 2 * CHUNK + CHUNK, CHUNK)], w1_sem.at[c, 1]),
        )

    def w1d_copy(c):
        slot = lax.rem(c, 2)
        return pltpu.make_async_copy(wd_hbm.at[1, cols(c), :], w1d.at[slot], w1d_sem.at[slot])

    squares[...] = jnp.zeros_like(squares)
    barrier = pltpu.get_barrier_semaphore()
    for away in range(1, n):
        pl.semaphore_signal(barrier, inc=1, device_id={AXIS: lax.rem(me + away, n)}, device_id_type=pl.DeviceIdType.MESH)

    first = (
        pltpu.make_async_copy(x_hbm.at[0, pl.ds(0, 2 * FTILE)], h1.at[pl.ds(0, 2 * FTILE)], first_sem.at[0]),
        pltpu.make_async_copy(wg_hbm.at[0], w0g, first_sem.at[1]),
        pltpu.make_async_copy(wu_hbm.at[0], w0u, first_sem.at[2]),
        pltpu.make_async_copy(wd_hbm.at[0], w0d, first_sem.at[3]),
        pltpu.make_async_copy(x_hbm.at[0, pl.ds(2 * FTILE, tokens - 2 * FTILE)], h1.at[pl.ds(2 * FTILE, tokens - 2 * FTILE)], first_sem.at[4]),
        pltpu.make_async_copy(dy_hbm.at[0], dy, first_sem.at[5]),
    )
    for copy in first[:3]:
        copy.start()

    def norm0(t):
        a = normed(h1[frows(t), :].astype(F32))
        a0[frows(t), :] = a
        a0t[:, frows(t)] = a.T

    def expand(t):
        a = a0[frows(t), :]
        for c in range(chunks):
            s = pl.ds(c * CHUNK, CHUNK)
            gate, up = mm(a, w0g[:, s]), mm(a, w0u[:, s])
            piece[:, pl.ds(pl.multiple_of(lax.rem(t, 2) * ff + c * CHUNK, CHUNK), CHUNK)] = (gate * sigmoid(gate) * up).astype(BF16)

    def contract(t):
        out = mm(piece[:, pl.ds(pl.multiple_of(lax.rem(t, 2) * ff, CHUNK), ff)], w0d[...])
        h = (h1[frows(t), :].astype(F32) + out.astype(BF16).astype(F32)).astype(BF16)
        h1[frows(t), :] = h
        a = normed(h.astype(F32))
        a1[frows(t), :] = a
        a1t[:, frows(t)] = a.T

    first[0].wait()
    for copy in first[3:5]:
        copy.start()
    norm0(0)
    norm0(1)
    first[1].wait()
    first[2].wait()
    for copy in first[5:]:
        copy.start()
    for c in range(chunks):
        for copy in w1_copies(c):
            copy.start()
        if c < 2:
            w1d_copy(c).start()
    expand(0)
    accd[...] = jnp.zeros_like(accd)
    accgu[...] = jnp.zeros_like(accgu)
    first[3].wait()
    first[4].wait()

    def forward(t, _):
        contract(t)
        expand(t + 1)
        norm0(jnp.minimum(t + 2, ftiles - 1))
        return 0

    lax.fori_loop(0, ftiles - 1, forward, 0)
    contract(ftiles - 1)
    first[5].wait()
    pl.semaphore_wait(barrier, n - 1)

    def elementwise(gate, up, dact, b):
        s = sigmoid(gate)
        p = gate * s
        act[...] = (p * up).astype(BF16)
        dact = dact.astype(BF16).astype(F32)
        dgu[b, :, CHUNK:] = (dact * p).astype(BF16)
        dgu[b, :, :CHUNK] = (dact * up * (s + p * (1.0 - s))).astype(BF16)

    def finish(g):
        rd, rf, to_group = d // n, CHUNK // n, place(g)
        for r in range(n):
            at = r * shard_rows
            grads[to_group, at : at + rd, :] = accgu[r * rd : (r + 1) * rd, :CHUNK].astype(BF16)
            grads[to_group, at + rd : at + 2 * rd, :] = accgu[r * rd : (r + 1) * rd, CHUNK:].astype(BF16)
            for q in range(d // CHUNK):
                grads[to_group, at + 2 * rd + q * rf : at + 2 * rd + (q + 1) * rf, :] = accd[r * rf : (r + 1) * rf, q * CHUNK : (q + 1) * CHUNK].astype(BF16)
        accd[...] = jnp.zeros_like(accd)
        accgu[...] = jnp.zeros_like(accgu)

    def kept(i):
        c, t, b = i // tiles, lax.rem(i, tiles), lax.rem(i, 2)
        return pltpu.make_async_copy(dgu.at[b], kept_hbm.at[rows(t), both(c)], keep_sem.at[b])

    def front1(i, b):
        c, t = i // tiles, lax.rem(i, tiles)
        a = a1[rows(t), :]
        w = w1[:, both(c)]
        elementwise(mm(a, w[:, :CHUNK]), mm(a, w[:, CHUNK:]), mm_nt(dy[rows(t), :], w1d[lax.rem(c, 2)]), b)

    def layer1(i, _):
        c, t, b = i // tiles, lax.rem(i, tiles), lax.rem(i, 2)

        @pl.when((t == tiles - 1) & (c + 1 < chunks))
        def _():
            for copy in w1_copies(c + 1):
                copy.wait()
            w1d_copy(c + 1).wait()

        kept(i).start()

        @pl.when(i > 0)
        def _():
            kept(i - 1).wait()

        accgu[...] += mm(a1t[:, rows(t)], dgu[b])
        accd[...] += mm_tn(act[...], dy[rows(t), :])
        front1(jnp.minimum(i + 1, total - 1), 1 - b)

        @pl.when(t == tiles - 1)
        def _():
            finish(c)

            @pl.when(c + 2 < chunks)
            def _():
                w1d_copy(c + 2).start()

        tick(i)
        return 0

    for copy in w1_copies(0):
        copy.wait()
    w1d_copy(0).wait()
    front1(0, 0)
    lax.fori_loop(0, total, layer1, 0)
    kept(total - 1).wait()

    def piece_copy(t, place):
        return pltpu.make_async_copy(kept_hbm.at[frows(t), :], place, piece_sem.at[lax.rem(t, 2)])

    def through_norm(t):
        by_a = accgu[...].astype(BF16).astype(F32)
        wide = h1[frows(t), :].astype(F32)
        scale = lax.rsqrt(jnp.mean(wide * wide, -1, keepdims=True) + 1e-6)
        along = jnp.sum(by_a * wide, -1, keepdims=True) * (scale * scale * scale / d)
        through = (by_a * scale - wide * along).astype(BF16).astype(F32)
        dy[frows(t), :] = (dy[frows(t), :].astype(F32) + through).astype(BF16)

    def between(k, _):
        for half_way, (place, other) in enumerate(((piece, a1t), (a1t, piece))):
            t = 2 * k + half_way
            piece_copy(t, place).wait()

            @pl.when(t + 1 < ftiles)
            def _():
                piece_copy(t + 1, other).start()

            product = mm_nt(place[...], w1[...])
            if half_way:
                through_norm(t - 1)
            else:
                pl.when(k > 0)(lambda: through_norm(t - 1))
            accgu[...] = product
            tick(total + t)
        return 0

    piece_copy(0, piece).start()
    lax.fori_loop(0, ftiles // 2, between, 0)
    through_norm(ftiles - 1)
    accgu[...] = jnp.zeros_like(accgu)

    def front0(i, b):
        c, t = i // tiles, lax.rem(i, tiles)
        a = a0[rows(t), :]
        elementwise(mm(a, w0g[:, cols(c)]), mm(a, w0u[:, cols(c)]), mm_nt(dy[rows(t), :], w0d[cols(c), :]), b)

    def layer0(i, _):
        c, t, b = i // tiles, lax.rem(i, tiles), lax.rem(i, 2)
        accgu[...] += mm(a0t[:, rows(t)], dgu[b])
        accd[...] += mm_tn(act[...], dy[rows(t), :])
        front0(jnp.minimum(i + 1, total - 1), 1 - b)

        @pl.when(t == tiles - 1)
        def _():
            finish(chunks + c)

        tick(total + ftiles + i)
        return 0

    front0(0, 0)
    lax.fori_loop(0, total, layer0, 0)

    def sq_copy(away, mine):
        q = me if mine else lax.rem(me + away, n)
        return pltpu.make_async_remote_copy(
            src_ref=squares.at[0], dst_ref=squares.at[1 + q], send_sem=sq_send.at[away - 1], recv_sem=sq_recv.at[q],
            device_id={AXIS: lax.rem(me + away, n)}, device_id_type=pl.DeviceIdType.MESH)

    end = over - 1 + hops * SPACING
    chances = (ag_lag + 3 * e + 2 * hops * ((pairs + 1 - e) // 2) for e in range(2))
    last = max(end, over + 1 + 2 * (max(chances) - (chunks - 1 + ftiles // 2 + in_layer0)))

    def drain(i, _):
        tick(i)

        @pl.when(i == end)
        def _():
            for away in range(1, n):
                sq_copy(away, True).start()

        return 0

    lax.fori_loop(over, last + 1, drain, 0)
    for away in range(1, n):
        sq_copy(away, True).wait_send()
        sq_copy(away, False).wait_recv()
    squares[pl.ds(1 + me, 1)] = squares[0:1]
    everyone = squares[1]
    for q in range(1, n):
        everyone += squares[1 + q]
    mean = jnp.sum(jnp.sum(everyone, axis=1, keepdims=True), axis=0, keepdims=True) / (6 * d * ff)
    factor_ref[...] = jnp.broadcast_to(jnp.minimum(1.0, 0.5 * lax.rsqrt(mean + 1e-30)), factor_ref.shape)
    me_ref[0] = me
    for pair in range(pairs):
        full_copy(pair).wait()
    own_copy(groups - 1, 1).wait()


def gradients_of(n, x, dy, wg, wu, wd):
    _, tokens, d = x.shape
    _, ff, _ = wd.shape
    chunks, hops = ff // CHUNK, n // 2
    shard_rows = 3 * d // n
    v, dma = pltpu.VMEM, pltpu.SemaphoreType.DMA
    anyspace = pl.BlockSpec(memory_space=pl.ANY)
    return pl.pallas_call(
        functools.partial(gradients_body, n),
        out_shape=(
            jax.ShapeDtypeStruct((chunks, n * shard_rows, CHUNK), BF16),
            jax.ShapeDtypeStruct((chunks // 2, shard_rows, CHUNK), BF16),
            jax.ShapeDtypeStruct((chunks // 2, shard_rows, CHUNK), BF16),
            jax.ShapeDtypeStruct((8, 128), F32),
            jax.ShapeDtypeStruct((1,), jnp.int32),
            jax.ShapeDtypeStruct((tokens, 2 * ff), BF16),
        ),
        in_specs=[anyspace] * 5,
        out_specs=(anyspace, anyspace, anyspace, pl.BlockSpec(memory_space=pltpu.VMEM), pl.BlockSpec(memory_space=pltpu.SMEM), anyspace),
        scratch_shapes=[
            v((tokens, d), BF16), v((d, tokens), BF16), v((tokens, d), BF16), v((d, tokens), BF16),
            v((tokens, d), BF16), v((tokens, d), BF16),
            v((d, ff), BF16), v((d, ff), BF16), v((ff, d), BF16),
            v((d, 2 * ff), BF16), v((2, CHUNK, d), BF16),
            v((TILE, CHUNK), BF16), v((2, TILE, 2 * CHUNK), BF16), v((FTILE, 2 * ff), BF16),
            v((CHUNK, d), F32), v((d, 2 * CHUNK), F32),
            v((chunks + RING, n * shard_rows, CHUNK), BF16),
            v((2, hops, 2, shard_rows, CHUNK), BF16), v((2, hops - 1, shard_rows, CHUNK), BF16),
            v((n + 1, 8, CHUNK), F32),
            dma((6,)), dma((chunks, 2)), dma((2,)), dma((2, hops, 2)), dma((2, hops, 2)), dma((2, hops, 2, 2)), dma((2, hops, 2, 2)),
            dma((n - 1,)), dma((n,)), dma((chunks // 2,)), dma((chunks,)), dma((2,)), dma((2,)),
        ],
        compiler_params=pltpu.CompilerParams(vmem_limit_bytes=VMEM_LIMIT, collective_id=0, has_side_effects=True),
        name="gradients",
    )(x, dy, wg, wu, wd)


def adamw_update(factor, wmv, new, i, at, g):
    g = g.astype(F32) * factor
    w, m, v = (wmv[3 * k + i][at].astype(F32) for k in range(3))
    m = 0.9 * m + 0.1 * g
    v = 0.95 * v + 0.05 * g * g
    w = w - 0.02 * (m * lax.rsqrt(v + 1e-8) + 0.1 * w)
    for k, value in enumerate((w, m, v)):
        new[3 * k + i][at] = value.astype(new[3 * k + i].dtype)


def adamw_body(parts, me_ref, factor_ref, *refs):
    arrays = sum(parts)
    gs, wmv, new = refs[:arrays], refs[arrays : arrays + 9], refs[-9:]
    rd, rf = wmv[0].shape[1], wmv[2].shape[2]
    d = wmv[2].shape[3]
    step = pl.program_id(1)
    update = functools.partial(adamw_update, factor_ref[0:1, 0:1], wmv, new)
    for k, many in enumerate(parts):

        def shard(refs=gs[sum(parts[:k]) : sum(parts[: k + 1])]):
            c = 0
            for g_ref in refs:
                base = pl.multiple_of(step * rd, rd)
                for q in range(g_ref.shape[0]):
                    for i in range(2):
                        update(i, (0, slice(None), slice(c * CHUNK, (c + 1) * CHUNK)), g_ref[q, pl.ds(base + i * rd * STEPS, rd), :])
                    for p in range(d // CHUNK):
                        at = pl.multiple_of(2 * rd * STEPS + p * rf * STEPS + step * rf, rf)
                        update(2, (0, c, slice(None), slice(p * CHUNK, (p + 1) * CHUNK)), g_ref[q, pl.ds(at, rf), :])
                    c += 1

        if len(parts) == 1:
            shard()
        else:
            pl.when(pl.program_id(0) == k)(shard)


def adamw(name, n, layer, device, shards, parts, gs, g_specs, me, factor, wmv, before):
    layers, d, ff = wmv[0].shape
    chunks = ff // CHUNK
    rd, rf = d // n // STEPS, CHUNK // n // STEPS
    wide = pl.BlockSpec((1, rd, ff), lambda k, s, me: (layer, device(k, me[0]) * STEPS + s, 0))
    tall = pl.BlockSpec((1, chunks, rf, d), lambda k, s, me: (layer, 0, device(k, me[0]) * STEPS + s, 0))
    blocks = [wide, wide, tall] * 3
    count = 3 * d * ff * shards // n
    return pl.pallas_call(
        functools.partial(adamw_body, parts),
        grid_spec=pltpu.PrefetchScalarGridSpec(
            num_scalar_prefetch=1,
            grid=(shards, STEPS),
            in_specs=[pl.BlockSpec((8, 128), lambda k, s, me: (0, 0)), *g_specs, *blocks, *[pl.BlockSpec(memory_space=pl.ANY)] * len(before)],
            out_specs=blocks,
        ),
        out_shape=[jax.ShapeDtypeStruct(a.shape, a.dtype) for a in wmv],
        input_output_aliases={2 + len(gs) + 9 + i: i for i in range(len(before))},
        compiler_params=pltpu.CompilerParams(vmem_limit_bytes=VMEM_LIMIT, dimension_semantics=("arbitrary",) * 2),
        cost_estimate=pl.CostEstimate(flops=400 * count, bytes_accessed=22 * count, transcendentals=count),
        name=name,
    )(me, factor, *gs, *wmv, *before)


def adamw_gathered(n, layer, lo, hi, g, me, factor, wmv, before):
    spec = pl.BlockSpec((g.shape[0], g.shape[1] // n, CHUNK), lambda k, s, me: (0, lo + k, 0))
    return adamw(f"adamw_{layer}_{lo}", n, layer, lambda k, me: lo + k, hi - lo, (1,), (g,), [spec], me, factor, wmv, before)


def adamw_shards(n, layer, aways, arrays, me, factor, wmv, before):
    def device(k, me):
        away = aways[-1]
        for i, other in enumerate(aways[:-1]):
            away = jnp.where(k == i, other, away)
        return lax.rem(me + away + n, n)

    gs = [g for some in arrays for g in some]
    specs = [pl.BlockSpec(g.shape, lambda k, s, me: (0, 0, 0)) for g in gs]
    return adamw(f"adamw_{layer}_{len(aways)}_{n + aways[0]}", n, layer, device, len(aways), tuple(len(some) for some in arrays), gs, specs, me, factor, wmv, before)


def solution(mesh):
    n = mesh.shape[AXIS]
    hops = n // 2
    right = [(i, (i + 1) % n) for i in range(n)]
    left = [(i, (i - 1) % n) for i in range(n)]

    def step(x, dy, *wmv):
        full, *own, factor, me, _ = gradients_of(n, x, dy, *wmv[:3])
        layers, d, ff = wmv[0].shape
        wmv = [a.reshape(layers, ff // CHUNK, CHUNK, d) if i % 3 == 2 else a for i, a in enumerate(wmv)]

        def permuted(arrays, pairs):
            return [lax.ppermute(a, AXIS, pairs) for a in arrays]

        a, b = permuted(own, right), permuted(own, left)
        most = n - n // 4
        new = adamw_gathered(n, 1, 0, most, full, me, factor, wmv, ())
        (a, b), new = lax.optimization_barrier(((a, b), new))
        aways, arrays = (0, -1, 1), (own, a, b)
        for j in range(1, hops):
            a, b = (permuted(a, right), permuted(b, left)) if j < hops - 1 else (permuted(a[:1], right), permuted(b[1:], left))
            if j == 1:
                new = adamw_gathered(n, 1, most, n, full, me, factor, wmv, new)
            new = adamw_shards(n, 0, aways, arrays, me, factor, wmv, new)
            (a, b), new = lax.optimization_barrier(((a, b), new))
            aways, arrays = (-1 - j, 1 + j), (a, b)
        new = adamw_shards(n, 0, (hops,), (a + b,), me, factor, wmv, new)
        return tuple(new_one.reshape(layers, ff, d) if i % 3 == 2 else new_one for i, new_one in enumerate(new))

    return jax.shard_map(
        step,
        mesh=mesh,
        in_specs=(P(("rep", "dp"), None, None),) * 2 + (P(None, None, None),) * 9,
        out_specs=(P("rep", None, None),) * 9,
        check_vma=False,
    )
```

```python
import functools

import jax
import jax.numpy as jnp
from jax import lax
from jax.experimental import pallas as pl
from jax.experimental.pallas import tpu as pltpu
from jax.sharding import PartitionSpec as P

F32, BF16 = jnp.float32, jnp.bfloat16
AXIS = "dp"
FTILE = 512
TILE = 1024
SPACING = 3
RING = 5
AG_SPACING = 6
CHUNK = 256
VMEM_LIMIT = 67043328


def mm(a, b):
    return jnp.dot(a, b, preferred_element_type=F32)


def mm_nt(a, b):
    return lax.dot_general(a, b, (((1,), (1,)), ((), ())), preferred_element_type=F32)


def mm_tn(a, b):
    return lax.dot_general(a, b, (((0,), (0,)), ((), ())), preferred_element_type=F32)


def sigmoid(x):
    return 0.5 * jnp.tanh(0.5 * x) + 0.5


def normed(wide):
    scale = lax.rsqrt(jnp.mean(wide * wide, -1, keepdims=True) + 1e-6)
    return (wide * scale).astype(BF16)


def gradients_body(n, x_hbm, dy_hbm, wg_hbm, wu_hbm, wd_hbm, full_hbm, own_hbm, factor_ref, me_ref, kept_hbm,
                   a0, a0t, a1, a1t, dy, h1, w0g, w0u, w0d, w1, w1d, act, dgu, piece, accd, accgu, grads, slots, sums, squares,
                   first_sem, w1_sem, w1d_sem, rs_send, rs_recv, ag_send, ag_recv, sq_send, sq_recv, full_sem, own_sem, keep_sem, piece_sem):
    tokens, d = h1.shape
    ff = w0d.shape[0]
    tiles, chunks = tokens // TILE, ff // CHUNK
    groups = 2 * chunks
    hops = n // 2
    shard_rows = grads.shape[1] // n
    half = shard_rows // 2
    me = lax.axis_index(AXIS)
    to = (lax.rem(me + 1, n), lax.rem(me + n - 1, n))

    def rows(t):
        return pl.ds(pl.multiple_of(t * TILE, TILE), TILE)

    def frows(t):
        return pl.ds(pl.multiple_of(t * FTILE, FTILE), FTILE)

    def cols(c):
        return pl.ds(pl.multiple_of(c * CHUNK, CHUNK), CHUNK)

    def shard(away):
        return pl.multiple_of(lax.rem(me + away + n, n) * shard_rows, shard_rows)

    def place(g):
        return jnp.where(g < chunks, g, chunks + lax.rem(g - chunks + RING, RING))

    def remote(src, dst, send, recv, way):
        return pltpu.make_async_remote_copy(src_ref=src, dst_ref=dst, send_sem=send, recv_sem=recv, device_id={AXIS: to[way]}, device_id_type=pl.DeviceIdType.MESH)

    def rs_copy(s, g, way):
        p = lax.rem(g, 2)
        if s == 1:
            part = pl.ds(way * half, half)
            src, dst = grads.at[place(g), pl.ds(shard(hops) + way * half, half)], slots.at[way, 0, p, part]
        else:
            src, dst = sums.at[way, s - 2], slots.at[way, s - 1, p]
        return remote(src, dst, rs_send.at[way, s - 1, p], rs_recv.at[way, s - 1, p], way)

    def rs_add(s, g):
        p = lax.rem(g, 2)
        for way in range(2):
            own = grads[place(g), pl.ds(shard((1 - 2 * way) * (hops + 1 - s)), shard_rows)]
            if s == 2:
                here = slice(way * half, way * half + half)
                there = slice(half - way * half, shard_rows - way * half)
                sums[way, 0, there] = own[there]
                sums[way, 0, here] = (slots[way, 0, p, here].astype(F32) + own[here].astype(F32)).astype(BF16)
            else:
                sums[way, s - 2] = (slots[way, s - 2, p].astype(F32) + own.astype(F32)).astype(BF16)

    def rs_final(g):
        p = lax.rem(g, 2)
        mine = pl.ds(shard(0), shard_rows)
        total = slots[0, hops - 1, p].astype(F32) + slots[1, hops - 1, p].astype(F32) + grads[place(g), mine].astype(F32)
        total = total.astype(BF16)
        grads[place(g), mine] = total
        wide = total.astype(F32)
        squares[0] += jnp.sum((wide * wide).reshape(shard_rows // 8, 8, CHUNK), axis=0)

    def ag_copies(pair, j, whole):
        copies = []
        for b in range(2):
            for way in range(2):
                at = shard((2 * way - 1) * j)
                part = pl.ds(at, shard_rows) if whole else pl.ds(at + way * half, half)
                ref = grads.at[2 * pair + b, part]
                copies.append(remote(ref, ref, ag_send.at[way, j, b, lax.rem(pair, 2)], ag_recv.at[way, j, b, lax.rem(pair, 2)], way))
        return copies

    def full_copy(pair):
        return pltpu.make_async_copy(grads.at[pl.ds(2 * pair, 2)], full_hbm.at[pl.ds(2 * pair, 2)], full_sem.at[pair])

    def own_copy(g):
        return pltpu.make_async_copy(grads.at[place(g), pl.ds(shard(0), shard_rows)], own_hbm.at[g - chunks], own_sem.at[g - chunks])

    pairs = chunks // 2

    total, ftiles = chunks * tiles, tokens // FTILE
    later = total + ftiles
    over = later + total

    ag_lag = -((2 - hops * SPACING) // tiles) + 1
    in_layer0 = (total - 2) // AG_SPACING + 1

    def tick(i):
        def group(s, f):
            step = i - (s - 1) * SPACING - (tiles - 1)
            last_layer = (step >= 0) & (step < total)
            first_layer = (step >= later) & (step < over)
            step = jnp.where(first_layer, step - ftiles, step)
            pl.when((last_layer | first_layer) & (lax.rem(step + tiles * groups, tiles) == 0))(functools.partial(f, step // tiles))

        def hop(s, g):
            if s > 1:
                for way in range(2):
                    rs_copy(s - 1, g, way).wait()
                rs_add(s, g)
            for way in range(2):
                rs_copy(s, g, way).start()

        def final(g):
            for way in range(2):
                rs_copy(hops, g, way).wait()
            rs_final(g)
            pl.when(g > chunks)(lambda: own_copy(g - 1).wait())
            pl.when(g >= chunks)(lambda: own_copy(g).start())

        group(hops + 1, final)
        for s in range(hops, 0, -1):
            group(s, functools.partial(hop, s))

        chance = jnp.where(
            i < total, i // tiles - 1, jnp.where(
                i < later, chunks - 1 + (i - total) // 2, jnp.where(
                    i < over, chunks - 1 + ftiles // 2 + (i - later) // AG_SPACING, chunks - 1 + ftiles // 2 + in_layer0 + (i - over) // 2)))
        due = jnp.where(
            i < total, lax.rem(i, tiles) == 1, jnp.where(
                i < later, lax.rem(i - total, 2) == 1, jnp.where(
                    i < over, lax.rem(i - later, AG_SPACING) == 1, lax.rem(i - over, 2) == 1)))
        chance = chance - ag_lag

        @pl.when(due & (chance >= 0))
        def _():
            e = lax.rem(chance + 2 * groups, 2)
            u = (chance - 3 * e) // 2

            def gathering(u, f):
                pair, j = 2 * (u // hops) + e, lax.rem(u + 2 * hops, hops)
                for whole in (True, False):
                    pl.when((chance >= 3 * e) & (u >= 0) & (pair < pairs) & ((j < hops - 1) == whole))(functools.partial(f, pair, j, whole))

            def landed(pair, j, whole):
                for copy in ag_copies(pair, j, whole):
                    copy.wait()
                if not whole:
                    full_copy(pair).start()

            def pass_on(pair, j, whole):
                for copy in ag_copies(pair, j, whole):
                    copy.start()

            gathering(u - 1, landed)
            gathering(u, pass_on)

    def both(c):
        return pl.ds(pl.multiple_of(c * 2 * CHUNK, 2 * CHUNK), 2 * CHUNK)

    def w1_copies(c):
        return (
            pltpu.make_async_copy(wg_hbm.at[1, :, cols(c)], w1.at[:, pl.ds(c * 2 * CHUNK, CHUNK)], w1_sem.at[c, 0]),
            pltpu.make_async_copy(wu_hbm.at[1, :, cols(c)], w1.at[:, pl.ds(c * 2 * CHUNK + CHUNK, CHUNK)], w1_sem.at[c, 1]),
        )

    def w1d_copy(c):
        slot = lax.rem(c, 2)
        return pltpu.make_async_copy(wd_hbm.at[1, cols(c), :], w1d.at[slot], w1d_sem.at[slot])

    squares[...] = jnp.zeros_like(squares)
    barrier = pltpu.get_barrier_semaphore()
    for away in range(1, n):
        pl.semaphore_signal(barrier, inc=1, device_id={AXIS: lax.rem(me + away, n)}, device_id_type=pl.DeviceIdType.MESH)

    first = (
        pltpu.make_async_copy(x_hbm.at[0, pl.ds(0, 2 * FTILE)], h1.at[pl.ds(0, 2 * FTILE)], first_sem.at[0]),
        pltpu.make_async_copy(wg_hbm.at[0], w0g, first_sem.at[1]),
        pltpu.make_async_copy(wu_hbm.at[0], w0u, first_sem.at[2]),
        pltpu.make_async_copy(wd_hbm.at[0], w0d, first_sem.at[3]),
        pltpu.make_async_copy(x_hbm.at[0, pl.ds(2 * FTILE, tokens - 2 * FTILE)], h1.at[pl.ds(2 * FTILE, tokens - 2 * FTILE)], first_sem.at[4]),
        pltpu.make_async_copy(dy_hbm.at[0], dy, first_sem.at[5]),
    )
    for copy in first[:3]:
        copy.start()

    def norm0(t):
        a = normed(h1[frows(t), :].astype(F32))
        a0[frows(t), :] = a
        a0t[:, frows(t)] = a.T

    def expand(t):
        a = a0[frows(t), :]
        for c in range(chunks):
            s = pl.ds(c * CHUNK, CHUNK)
            gate, up = mm(a, w0g[:, s]), mm(a, w0u[:, s])
            piece[:, pl.ds(pl.multiple_of(lax.rem(t, 2) * ff + c * CHUNK, CHUNK), CHUNK)] = (gate * sigmoid(gate) * up).astype(BF16)

    def contract(t):
        out = mm(piece[:, pl.ds(pl.multiple_of(lax.rem(t, 2) * ff, CHUNK), ff)], w0d[...])
        h = (h1[frows(t), :].astype(F32) + out.astype(BF16).astype(F32)).astype(BF16)
        h1[frows(t), :] = h
        a = normed(h.astype(F32))
        a1[frows(t), :] = a
        a1t[:, frows(t)] = a.T

    first[0].wait()
    for copy in first[3:5]:
        copy.start()
    norm0(0)
    norm0(1)
    first[1].wait()
    first[2].wait()
    for copy in first[5:]:
        copy.start()
    for c in range(chunks):
        for copy in w1_copies(c):
            copy.start()
        if c < 2:
            w1d_copy(c).start()
    expand(0)
    accd[...] = jnp.zeros_like(accd)
    accgu[...] = jnp.zeros_like(accgu)
    first[3].wait()
    first[4].wait()

    def forward(t, _):
        contract(t)
        expand(t + 1)
        norm0(jnp.minimum(t + 2, ftiles - 1))
        return 0

    lax.fori_loop(0, ftiles - 1, forward, 0)
    contract(ftiles - 1)
    first[5].wait()
    pl.semaphore_wait(barrier, n - 1)

    def elementwise(gate, up, dact, b):
        s = sigmoid(gate)
        p = gate * s
        act[...] = (p * up).astype(BF16)
        dact = dact.astype(BF16).astype(F32)
        dgu[b, :, CHUNK:] = (dact * p).astype(BF16)
        dgu[b, :, :CHUNK] = (dact * up * (s + p * (1.0 - s))).astype(BF16)

    def finish(g):
        rd, rf, to_group = d // n, CHUNK // n, place(g)
        for r in range(n):
            at = r * shard_rows
            grads[to_group, at : at + rd, :] = accgu[r * rd : (r + 1) * rd, :CHUNK].astype(BF16)
            grads[to_group, at + rd : at + 2 * rd, :] = accgu[r * rd : (r + 1) * rd, CHUNK:].astype(BF16)
            for q in range(d // CHUNK):
                grads[to_group, at + 2 * rd + q * rf : at + 2 * rd + (q + 1) * rf, :] = accd[r * rf : (r + 1) * rf, q * CHUNK : (q + 1) * CHUNK].astype(BF16)
        accd[...] = jnp.zeros_like(accd)
        accgu[...] = jnp.zeros_like(accgu)

    def kept(i):
        c, t, b = i // tiles, lax.rem(i, tiles), lax.rem(i, 2)
        return pltpu.make_async_copy(dgu.at[b], kept_hbm.at[rows(t), both(c)], keep_sem.at[b])

    def front1(i, b):
        c, t = i // tiles, lax.rem(i, tiles)
        a = a1[rows(t), :]
        w = w1[:, both(c)]
        elementwise(mm(a, w[:, :CHUNK]), mm(a, w[:, CHUNK:]), mm_nt(dy[rows(t), :], w1d[lax.rem(c, 2)]), b)

    def layer1(i, _):
        c, t, b = i // tiles, lax.rem(i, tiles), lax.rem(i, 2)

        @pl.when((t == tiles - 1) & (c + 1 < chunks))
        def _():
            for copy in w1_copies(c + 1):
                copy.wait()
            w1d_copy(c + 1).wait()

        kept(i).start()

        @pl.when(i > 0)
        def _():
            kept(i - 1).wait()

        accgu[...] += mm(a1t[:, rows(t)], dgu[b])
        accd[...] += mm_tn(act[...], dy[rows(t), :])
        front1(jnp.minimum(i + 1, total - 1), 1 - b)

        @pl.when(t == tiles - 1)
        def _():
            finish(c)

            @pl.when(c + 2 < chunks)
            def _():
                w1d_copy(c + 2).start()

        tick(i)
        return 0

    for copy in w1_copies(0):
        copy.wait()
    w1d_copy(0).wait()
    front1(0, 0)
    lax.fori_loop(0, total, layer1, 0)
    kept(total - 1).wait()

    def piece_copy(t, place):
        return pltpu.make_async_copy(kept_hbm.at[frows(t), :], place, piece_sem.at[lax.rem(t, 2)])

    def through_norm(t):
        by_a = accgu[...].astype(BF16).astype(F32)
        wide = h1[frows(t), :].astype(F32)
        scale = lax.rsqrt(jnp.mean(wide * wide, -1, keepdims=True) + 1e-6)
        along = jnp.sum(by_a * wide, -1, keepdims=True) * (scale * scale * scale / d)
        through = (by_a * scale - wide * along).astype(BF16).astype(F32)
        dy[frows(t), :] = (dy[frows(t), :].astype(F32) + through).astype(BF16)

    def between(k, _):
        for half_way, (place, other) in enumerate(((piece, a1t), (a1t, piece))):
            t = 2 * k + half_way
            piece_copy(t, place).wait()

            @pl.when(t + 1 < ftiles)
            def _():
                piece_copy(t + 1, other).start()

            product = mm_nt(place[...], w1[...])
            if half_way:
                through_norm(t - 1)
            else:
                pl.when(k > 0)(lambda: through_norm(t - 1))
            accgu[...] = product
            tick(total + t)
        return 0

    piece_copy(0, piece).start()
    lax.fori_loop(0, ftiles // 2, between, 0)
    through_norm(ftiles - 1)
    accgu[...] = jnp.zeros_like(accgu)

    def front0(i, b):
        c, t = i // tiles, lax.rem(i, tiles)
        a = a0[rows(t), :]
        elementwise(mm(a, w0g[:, cols(c)]), mm(a, w0u[:, cols(c)]), mm_nt(dy[rows(t), :], w0d[cols(c), :]), b)

    def layer0(i, _):
        c, t, b = i // tiles, lax.rem(i, tiles), lax.rem(i, 2)
        accgu[...] += mm(a0t[:, rows(t)], dgu[b])
        accd[...] += mm_tn(act[...], dy[rows(t), :])
        front0(jnp.minimum(i + 1, total - 1), 1 - b)

        @pl.when(t == tiles - 1)
        def _():
            finish(chunks + c)

        tick(total + ftiles + i)
        return 0

    front0(0, 0)
    lax.fori_loop(0, total, layer0, 0)

    def sq_copy(away, mine):
        q = me if mine else lax.rem(me + away, n)
        return pltpu.make_async_remote_copy(
            src_ref=squares.at[0], dst_ref=squares.at[1 + q], send_sem=sq_send.at[away - 1], recv_sem=sq_recv.at[q],
            device_id={AXIS: lax.rem(me + away, n)}, device_id_type=pl.DeviceIdType.MESH)

    end = over - 1 + hops * SPACING
    chances = (ag_lag + 3 * e + 2 * hops * ((pairs + 1 - e) // 2) for e in range(2))
    last = max(end, over + 1 + 2 * (max(chances) - (chunks - 1 + ftiles // 2 + in_layer0)))

    def drain(i, _):
        tick(i)

        @pl.when(i == end)
        def _():
            for away in range(1, n):
                sq_copy(away, True).start()

        return 0

    lax.fori_loop(over, last + 1, drain, 0)
    for away in range(1, n):
        sq_copy(away, True).wait_send()
        sq_copy(away, False).wait_recv()
    squares[pl.ds(1 + me, 1)] = squares[0:1]
    everyone = squares[1]
    for q in range(1, n):
        everyone += squares[1 + q]
    mean = jnp.sum(jnp.sum(everyone, axis=1, keepdims=True), axis=0, keepdims=True) / (6 * d * ff)
    factor_ref[...] = jnp.broadcast_to(jnp.minimum(1.0, 0.5 * lax.rsqrt(mean + 1e-30)), factor_ref.shape)
    me_ref[0] = me
    for pair in range(pairs):
        full_copy(pair).wait()
    own_copy(groups - 1).wait()


def gradients_of(n, x, dy, wg, wu, wd):
    _, tokens, d = x.shape
    _, ff, _ = wd.shape
    chunks, hops = ff // CHUNK, n // 2
    shard_rows = 3 * d // n
    v, dma = pltpu.VMEM, pltpu.SemaphoreType.DMA
    anyspace = pl.BlockSpec(memory_space=pl.ANY)
    return pl.pallas_call(
        functools.partial(gradients_body, n),
        out_shape=(
            jax.ShapeDtypeStruct((chunks, n * shard_rows, CHUNK), BF16),
            jax.ShapeDtypeStruct((chunks, shard_rows, CHUNK), BF16),
            jax.ShapeDtypeStruct((8, 128), F32),
            jax.ShapeDtypeStruct((1,), jnp.int32),
            jax.ShapeDtypeStruct((tokens, 2 * ff), BF16),
        ),
        in_specs=[anyspace] * 5,
        out_specs=(anyspace, anyspace, pl.BlockSpec(memory_space=pltpu.VMEM), pl.BlockSpec(memory_space=pltpu.SMEM), anyspace),
        scratch_shapes=[
            v((tokens, d), BF16), v((d, tokens), BF16), v((tokens, d), BF16), v((d, tokens), BF16),
            v((tokens, d), BF16), v((tokens, d), BF16),
            v((d, ff), BF16), v((d, ff), BF16), v((ff, d), BF16),
            v((d, 2 * ff), BF16), v((2, CHUNK, d), BF16),
            v((TILE, CHUNK), BF16), v((2, TILE, 2 * CHUNK), BF16), v((FTILE, 2 * ff), BF16),
            v((CHUNK, d), F32), v((d, 2 * CHUNK), F32),
            v((chunks + RING, n * shard_rows, CHUNK), BF16),
            v((2, hops, 2, shard_rows, CHUNK), BF16), v((2, hops - 1, shard_rows, CHUNK), BF16),
            v((n + 1, 8, CHUNK), F32),
            dma((6,)), dma((chunks, 2)), dma((2,)), dma((2, hops, 2)), dma((2, hops, 2)), dma((2, hops, 2, 2)), dma((2, hops, 2, 2)),
            dma((n - 1,)), dma((n,)), dma((chunks // 2,)), dma((chunks,)), dma((2,)), dma((2,)),
        ],
        compiler_params=pltpu.CompilerParams(vmem_limit_bytes=VMEM_LIMIT, collective_id=0, has_side_effects=True),
        name="gradients",
    )(x, dy, wg, wu, wd)


def adamw_update(factor, wmv, new, i, at, g):
    g = g.astype(F32) * factor
    w, m, v = (wmv[3 * k + i][at].astype(F32) for k in range(3))
    m = 0.9 * m + 0.1 * g
    v = 0.95 * v + 0.05 * g * g
    w = w - 0.02 * (m * lax.rsqrt(v + 1e-8) + 0.1 * w)
    for k, value in enumerate((w, m, v)):
        new[3 * k + i][at] = value.astype(new[3 * k + i].dtype)


def adamw_body(parts, steps, me_ref, factor_ref, *refs):
    arrays = sum(parts)
    gs, wmv, new = refs[:arrays], refs[arrays : arrays + 9], refs[-9:]
    rd, rf = wmv[0].shape[1], wmv[2].shape[2]
    d = wmv[2].shape[3]
    step = pl.program_id(1)
    update = functools.partial(adamw_update, factor_ref[0:1, 0:1], wmv, new)
    for k, many in enumerate(parts):

        def shard(refs=gs[sum(parts[:k]) : sum(parts[: k + 1])]):
            c = 0
            for g_ref in refs:
                base = pl.multiple_of(step * rd, rd)
                for q in range(g_ref.shape[0]):
                    for i in range(2):
                        update(i, (0, slice(None), slice(c * CHUNK, (c + 1) * CHUNK)), g_ref[q, pl.ds(base + i * rd * steps, rd), :])
                    for p in range(d // CHUNK):
                        at = pl.multiple_of(2 * rd * steps + p * rf * steps + step * rf, rf)
                        update(2, (0, c, slice(None), slice(p * CHUNK, (p + 1) * CHUNK)), g_ref[q, pl.ds(at, rf), :])
                    c += 1

        if len(parts) == 1:
            shard()
        else:
            pl.when(pl.program_id(0) == k)(shard)


def adamw(name, n, layer, device, shards, parts, gs, g_specs, me, factor, wmv, before):
    layers, d, ff = wmv[0].shape
    chunks = ff // CHUNK
    steps = 2 if shards == 1 else 1
    rd, rf = d // n // steps, CHUNK // n // steps
    wide = pl.BlockSpec((1, rd, ff), lambda k, s, me: (layer, device(k, me[0]) * steps + s, 0))
    tall = pl.BlockSpec((1, chunks, rf, d), lambda k, s, me: (layer, 0, device(k, me[0]) * steps + s, 0))
    blocks = [wide, wide, tall] * 3
    count = 3 * d * ff * shards // n
    return pl.pallas_call(
        functools.partial(adamw_body, parts, steps),
        grid_spec=pltpu.PrefetchScalarGridSpec(
            num_scalar_prefetch=1,
            grid=(shards, steps),
            in_specs=[pl.BlockSpec((8, 128), lambda k, s, me: (0, 0)), *g_specs, *blocks, *[pl.BlockSpec(memory_space=pl.ANY)] * len(before)],
            out_specs=blocks,
        ),
        out_shape=[jax.ShapeDtypeStruct(a.shape, a.dtype) for a in wmv],
        input_output_aliases={2 + len(gs) + 9 + i: i for i in range(len(before))},
        compiler_params=pltpu.CompilerParams(vmem_limit_bytes=VMEM_LIMIT, dimension_semantics=("arbitrary",) * 2),
        cost_estimate=pl.CostEstimate(flops=400 * count, bytes_accessed=22 * count, transcendentals=count),
        name=name,
    )(me, factor, *gs, *wmv, *before)


def adamw_gathered(n, layer, lo, hi, g, me, factor, wmv, before):
    spec = pl.BlockSpec((g.shape[0], g.shape[1] // n, CHUNK), lambda k, s, me: (0, lo + k, 0))
    return adamw(f"adamw_{layer}_{lo}", n, layer, lambda k, me: lo + k, hi - lo, (1,), (g,), [spec], me, factor, wmv, before)


def adamw_shards(n, layer, aways, arrays, me, factor, wmv, before):
    def device(k, me):
        away = aways[-1]
        for i, other in enumerate(aways[:-1]):
            away = jnp.where(k == i, other, away)
        return lax.rem(me + away + n, n)

    gs = [g for some in arrays for g in some]
    specs = [pl.BlockSpec(g.shape, lambda k, s, me: (0, 0, 0)) for g in gs]
    return adamw(f"adamw_{layer}_{len(aways)}_{n + aways[0]}", n, layer, device, len(aways), tuple(len(some) for some in arrays), gs, specs, me, factor, wmv, before)


def halves(a, b):
    def copy(a_ref, b_ref, first_ref, second_ref):
        first_ref[...] = a_ref[...]
        second_ref[...] = b_ref[...]

    half = (a.shape[0] // 2, *a.shape[1:])
    zero = (0,) * (a.ndim - 1)
    return pl.pallas_call(
        copy,
        grid=(1,),
        out_shape=[jax.ShapeDtypeStruct(half, a.dtype)] * 2,
        in_specs=[pl.BlockSpec(half, lambda k: (0, *zero)), pl.BlockSpec(half, lambda k: (1, *zero))],
        out_specs=[pl.BlockSpec(half, lambda k: (0, *zero))] * 2,
        compiler_params=pltpu.CompilerParams(vmem_limit_bytes=VMEM_LIMIT),
        name="halves",
    )(a, b)


def solution(mesh):
    n = mesh.shape[AXIS]
    hops = n // 2
    right = [(i, (i + 1) % n) for i in range(n)]
    left = [(i, (i - 1) % n) for i in range(n)]

    def step(x, dy, *wmv):
        full, own, factor, me, _ = gradients_of(n, x, dy, *wmv[:3])
        layers, d, ff = wmv[0].shape
        chunks = ff // CHUNK
        wmv = [a.reshape(layers, chunks, CHUNK, d) if i % 3 == 2 else a for i, a in enumerate(wmv)]

        a, b = lax.ppermute(own, AXIS, right), lax.ppermute(own, AXIS, left)
        most = n - n // 4 - 1
        new = adamw_gathered(n, 1, 0, most, full, me, factor, wmv, ())
        (a, b), new = lax.optimization_barrier(((a, b), new))
        ready, some = (0,), (own,)
        for j in range(1, hops):
            ready, some = ready + (-j, j), some + (a, b)
            if j == hops - 1:
                a, b = halves(a, b)
            a, b = lax.ppermute(a, AXIS, right), lax.ppermute(b, AXIS, left)
            if j == 1:
                new = adamw_gathered(n, 1, most, n, full, me, factor, wmv, new)
            take = 1 if j == 1 else 4 if j == 2 else len(ready)
            new = adamw_shards(n, 0, ready[:take], [(g,) for g in some[:take]], me, factor, wmv, new)
            ready, some = ready[take:], some[take:]
            (a, b), new, some = lax.optimization_barrier(((a, b), new, some))
        new = adamw_shards(n, 0, (*ready, hops), [*[(g,) for g in some], (a, b)], me, factor, wmv, new)
        return tuple(new_one.reshape(layers, ff, d) if i % 3 == 2 else new_one for i, new_one in enumerate(new))

    return jax.shard_map(
        step,
        mesh=mesh,
        in_specs=(P(("rep", "dp"), None, None),) * 2 + (P(None, None, None),) * 9,
        out_specs=(P("rep", None, None),) * 9,
        check_vma=False,
    )
```

```python
import functools

import jax
import jax.numpy as jnp
from jax import lax
from jax.experimental import pallas as pl
from jax.experimental.pallas import tpu as pltpu
from jax.sharding import PartitionSpec as P

F32, BF16 = jnp.float32, jnp.bfloat16
AXIS = "dp"
FTILE = 512
TILE = 1024
SPACING = 3
RING = 5
AG_SPACING = 6
CHUNK = 256
VMEM_LIMIT = 67043328


def mm(a, b):
    return jnp.dot(a, b, preferred_element_type=F32)


def mm_nt(a, b):
    return lax.dot_general(a, b, (((1,), (1,)), ((), ())), preferred_element_type=F32)


def mm_tn(a, b):
    return lax.dot_general(a, b, (((0,), (0,)), ((), ())), preferred_element_type=F32)


def sigmoid(x):
    return 0.5 * jnp.tanh(0.5 * x) + 0.5


def normed(wide):
    scale = lax.rsqrt(jnp.mean(wide * wide, -1, keepdims=True) + 1e-6)
    return (wide * scale).astype(BF16)


def gradients_body(n, x_hbm, dy_hbm, wg_hbm, wu_hbm, wd_hbm, full_hbm, own_hbm, factor_ref, me_ref, kept_hbm,
                   a0, a0t, a1, a1t, dy, h1, w0g, w0u, w0d, w1, w1d, act, dgu, piece, accd, accgu, grads, slots, sums, squares,
                   first_sem, w1_sem, w1d_sem, rs_send, rs_recv, ag_send, ag_recv, sq_send, sq_recv, full_sem, own_sem, keep_sem, piece_sem):
    tokens, d = h1.shape
    ff = w0d.shape[0]
    tiles, chunks = tokens // TILE, ff // CHUNK
    groups = 2 * chunks
    hops = n // 2
    shard_rows = grads.shape[1] // n
    half = shard_rows // 2
    me = lax.axis_index(AXIS)
    to = (lax.rem(me + 1, n), lax.rem(me + n - 1, n))

    def rows(t):
        return pl.ds(pl.multiple_of(t * TILE, TILE), TILE)

    def frows(t):
        return pl.ds(pl.multiple_of(t * FTILE, FTILE), FTILE)

    def cols(c):
        return pl.ds(pl.multiple_of(c * CHUNK, CHUNK), CHUNK)

    def shard(away):
        return pl.multiple_of(lax.rem(me + away + n, n) * shard_rows, shard_rows)

    def place(g):
        return jnp.where(g < chunks, g, chunks + lax.rem(g - chunks + RING, RING))

    def remote(src, dst, send, recv, way):
        return pltpu.make_async_remote_copy(src_ref=src, dst_ref=dst, send_sem=send, recv_sem=recv, device_id={AXIS: to[way]}, device_id_type=pl.DeviceIdType.MESH)

    def rs_copy(s, g, way):
        p = lax.rem(g, 2)
        if s == 1:
            part = pl.ds(way * half, half)
            src, dst = grads.at[place(g), pl.ds(shard(hops) + way * half, half)], slots.at[way, 0, p, part]
        else:
            src, dst = sums.at[way, s - 2], slots.at[way, s - 1, p]
        return remote(src, dst, rs_send.at[way, s - 1, p], rs_recv.at[way, s - 1, p], way)

    def rs_add(s, g):
        p = lax.rem(g, 2)
        for way in range(2):
            own = grads[place(g), pl.ds(shard((1 - 2 * way) * (hops + 1 - s)), shard_rows)]
            if s == 2:
                here = slice(way * half, way * half + half)
                there = slice(half - way * half, shard_rows - way * half)
                sums[way, 0, there] = own[there]
                sums[way, 0, here] = (slots[way, 0, p, here].astype(F32) + own[here].astype(F32)).astype(BF16)
            else:
                sums[way, s - 2] = (slots[way, s - 2, p].astype(F32) + own.astype(F32)).astype(BF16)

    def rs_final(g):
        p = lax.rem(g, 2)
        mine = pl.ds(shard(0), shard_rows)
        total = slots[0, hops - 1, p].astype(F32) + slots[1, hops - 1, p].astype(F32) + grads[place(g), mine].astype(F32)
        total = total.astype(BF16)
        grads[place(g), mine] = total
        wide = total.astype(F32)
        squares[0] += jnp.sum((wide * wide).reshape(shard_rows // 8, 8, CHUNK), axis=0)

    def ag_copies(pair, j, whole):
        copies = []
        for b in range(2):
            for way in range(2):
                at = shard((2 * way - 1) * j)
                part = pl.ds(at, shard_rows) if whole else pl.ds(at + way * half, half)
                ref = grads.at[2 * pair + b, part]
                copies.append(remote(ref, ref, ag_send.at[way, j, b, lax.rem(pair, 2)], ag_recv.at[way, j, b, lax.rem(pair, 2)], way))
        return copies

    def full_copy(pair):
        return pltpu.make_async_copy(grads.at[pl.ds(2 * pair, 2)], full_hbm.at[pl.ds(2 * pair, 2)], full_sem.at[pair])

    def own_copy(g):
        return pltpu.make_async_copy(grads.at[place(g), pl.ds(shard(0), shard_rows)], own_hbm.at[g - chunks], own_sem.at[g - chunks])

    pairs = chunks // 2

    total, ftiles = chunks * tiles, tokens // FTILE
    later = total + ftiles
    over = later + total

    ag_lag = -((2 - hops * SPACING) // tiles) + 1
    in_layer0 = (total - 2) // AG_SPACING + 1

    def tick(i):
        def group(s, f):
            step = i - (s - 1) * SPACING - (tiles - 1)
            last_layer = (step >= 0) & (step < total)
            first_layer = (step >= later) & (step < over)
            step = jnp.where(first_layer, step - ftiles, step)
            pl.when((last_layer | first_layer) & (lax.rem(step + tiles * groups, tiles) == 0))(functools.partial(f, step // tiles))

        def hop(s, g):
            if s > 1:
                for way in range(2):
                    rs_copy(s - 1, g, way).wait()
                rs_add(s, g)
            for way in range(2):
                rs_copy(s, g, way).start()

        def final(g):
            for way in range(2):
                rs_copy(hops, g, way).wait()
            rs_final(g)
            pl.when(g > chunks)(lambda: own_copy(g - 1).wait())
            pl.when(g >= chunks)(lambda: own_copy(g).start())

        group(hops + 1, final)
        for s in range(hops, 0, -1):
            group(s, functools.partial(hop, s))

        chance = jnp.where(
            i < total, i // tiles - 1, jnp.where(
                i < later, chunks - 1 + (i - total) // 2, jnp.where(
                    i < over, chunks - 1 + ftiles // 2 + (i - later) // AG_SPACING, chunks - 1 + ftiles // 2 + in_layer0 + (i - over) // 2)))
        due = jnp.where(
            i < total, lax.rem(i, tiles) == 1, jnp.where(
                i < later, lax.rem(i - total, 2) == 1, jnp.where(
                    i < over, lax.rem(i - later, AG_SPACING) == 1, lax.rem(i - over, 2) == 1)))
        chance = chance - ag_lag

        @pl.when(due & (chance >= 0))
        def _():
            e = lax.rem(chance + 2 * groups, 2)
            u = (chance - 3 * e) // 2

            def gathering(u, f):
                pair, j = 2 * (u // hops) + e, lax.rem(u + 2 * hops, hops)
                for whole in (True, False):
                    pl.when((chance >= 3 * e) & (u >= 0) & (pair < pairs) & ((j < hops - 1) == whole))(functools.partial(f, pair, j, whole))

            def landed(pair, j, whole):
                for copy in ag_copies(pair, j, whole):
                    copy.wait()
                if not whole:
                    full_copy(pair).start()

            def pass_on(pair, j, whole):
                for copy in ag_copies(pair, j, whole):
                    copy.start()

            gathering(u - 1, landed)
            gathering(u, pass_on)

    def both(c):
        return pl.ds(pl.multiple_of(c * 2 * CHUNK, 2 * CHUNK), 2 * CHUNK)

    def w1_copies(c):
        return (
            pltpu.make_async_copy(wg_hbm.at[1, :, cols(c)], w1.at[:, pl.ds(c * 2 * CHUNK, CHUNK)], w1_sem.at[c, 0]),
            pltpu.make_async_copy(wu_hbm.at[1, :, cols(c)], w1.at[:, pl.ds(c * 2 * CHUNK + CHUNK, CHUNK)], w1_sem.at[c, 1]),
        )

    def w1d_copy(c):
        slot = lax.rem(c, 2)
        return pltpu.make_async_copy(wd_hbm.at[1, cols(c), :], w1d.at[slot], w1d_sem.at[slot])

    squares[...] = jnp.zeros_like(squares)
    barrier = pltpu.get_barrier_semaphore()
    for away in range(1, n):
        pl.semaphore_signal(barrier, inc=1, device_id={AXIS: lax.rem(me + away, n)}, device_id_type=pl.DeviceIdType.MESH)

    first = (
        *(pltpu.make_async_copy(x_hbm.at[0, part], h1.at[part], first_sem.at[k]) for k, part in enumerate((pl.ds(0, FTILE), pl.ds(FTILE, FTILE), pl.ds(2 * FTILE, tokens - 2 * FTILE)))),
        *(pltpu.make_async_copy(src.at[0, :, pl.ds(k * ff // 2, ff // 2)], dst.at[:, pl.ds(k * ff // 2, ff // 2)], first_sem.at[3 + 2 * k + q])
          for k in range(2) for q, (src, dst) in enumerate(((wg_hbm, w0g), (wu_hbm, w0u)))),
        pltpu.make_async_copy(wd_hbm.at[0], w0d, first_sem.at[7]),
        pltpu.make_async_copy(dy_hbm.at[0], dy, first_sem.at[8]),
    )
    for k in (0, 3, 4, 1, 5, 6):
        first[k].start()

    def norm0(t):
        a = normed(h1[frows(t), :].astype(F32))
        a0[frows(t), :] = a
        a0t[:, frows(t)] = a.T

    def expand(t, lo=0, hi=chunks):
        a = a0[frows(t), :]
        for c in range(lo, hi):
            s = pl.ds(c * CHUNK, CHUNK)
            gate, up = mm(a, w0g[:, s]), mm(a, w0u[:, s])
            piece[:, pl.ds(pl.multiple_of(lax.rem(t, 2) * ff + c * CHUNK, CHUNK), CHUNK)] = (gate * sigmoid(gate) * up).astype(BF16)

    def contract(t):
        out = mm(piece[:, pl.ds(pl.multiple_of(lax.rem(t, 2) * ff, CHUNK), ff)], w0d[...])
        h = (h1[frows(t), :].astype(F32) + out.astype(BF16).astype(F32)).astype(BF16)
        h1[frows(t), :] = h
        a = normed(h.astype(F32))
        a1[frows(t), :] = a
        a1t[:, frows(t)] = a.T

    first[0].wait()
    norm0(0)
    first[3].wait()
    first[4].wait()
    expand(0, 0, chunks // 2)
    for k in (1, 5, 6):
        first[k].wait()
    for k in (7, 2, 8):
        first[k].start()
    for c in range(chunks):
        for copy in w1_copies(c):
            copy.start()
        if c < 2:
            w1d_copy(c).start()
    expand(0, chunks // 2, chunks)
    norm0(1)
    accd[...] = jnp.zeros_like(accd)
    accgu[...] = jnp.zeros_like(accgu)
    first[7].wait()
    first[2].wait()

    def forward(t, _):
        contract(t)
        expand(t + 1)
        norm0(jnp.minimum(t + 2, ftiles - 1))
        return 0

    lax.fori_loop(0, ftiles - 1, forward, 0)
    contract(ftiles - 1)
    first[8].wait()
    pl.semaphore_wait(barrier, n - 1)

    def elementwise(gate, up, dact, b):
        s = sigmoid(gate)
        p = gate * s
        act[...] = (p * up).astype(BF16)
        dact = dact.astype(BF16).astype(F32)
        dgu[b, :, CHUNK:] = (dact * p).astype(BF16)
        dgu[b, :, :CHUNK] = (dact * up * (s + p * (1.0 - s))).astype(BF16)

    def finish(g):
        rd, rf, to_group = d // n, CHUNK // n, place(g)
        for r in range(n):
            at = r * shard_rows
            grads[to_group, at : at + rd, :] = accgu[r * rd : (r + 1) * rd, :CHUNK].astype(BF16)
            grads[to_group, at + rd : at + 2 * rd, :] = accgu[r * rd : (r + 1) * rd, CHUNK:].astype(BF16)
            for q in range(d // CHUNK):
                grads[to_group, at + 2 * rd + q * rf : at + 2 * rd + (q + 1) * rf, :] = accd[r * rf : (r + 1) * rf, q * CHUNK : (q + 1) * CHUNK].astype(BF16)
        accd[...] = jnp.zeros_like(accd)
        accgu[...] = jnp.zeros_like(accgu)

    def kept(i):
        c, t, b = i // tiles, lax.rem(i, tiles), lax.rem(i, 2)
        return pltpu.make_async_copy(dgu.at[b], kept_hbm.at[rows(t), both(c)], keep_sem.at[b])

    def front1(i, b):
        c, t = i // tiles, lax.rem(i, tiles)
        a = a1[rows(t), :]
        w = w1[:, both(c)]
        elementwise(mm(a, w[:, :CHUNK]), mm(a, w[:, CHUNK:]), mm_nt(dy[rows(t), :], w1d[lax.rem(c, 2)]), b)

    def layer1(i, _):
        c, t, b = i // tiles, lax.rem(i, tiles), lax.rem(i, 2)

        @pl.when((t == tiles - 1) & (c + 1 < chunks))
        def _():
            for copy in w1_copies(c + 1):
                copy.wait()
            w1d_copy(c + 1).wait()

        kept(i).start()

        @pl.when(i > 0)
        def _():
            kept(i - 1).wait()

        accgu[...] += mm(a1t[:, rows(t)], dgu[b])
        accd[...] += mm_tn(act[...], dy[rows(t), :])
        front1(jnp.minimum(i + 1, total - 1), 1 - b)

        @pl.when(t == tiles - 1)
        def _():
            finish(c)

            @pl.when(c + 2 < chunks)
            def _():
                w1d_copy(c + 2).start()

        tick(i)
        return 0

    for copy in w1_copies(0):
        copy.wait()
    w1d_copy(0).wait()
    front1(0, 0)
    lax.fori_loop(0, total, layer1, 0)
    kept(total - 1).wait()

    def piece_copy(t, place):
        return pltpu.make_async_copy(kept_hbm.at[frows(t), :], place, piece_sem.at[lax.rem(t, 2)])

    def through_norm(t):
        by_a = accgu[...].astype(BF16).astype(F32)
        wide = h1[frows(t), :].astype(F32)
        scale = lax.rsqrt(jnp.mean(wide * wide, -1, keepdims=True) + 1e-6)
        along = jnp.sum(by_a * wide, -1, keepdims=True) * (scale * scale * scale / d)
        through = (by_a * scale - wide * along).astype(BF16).astype(F32)
        dy[frows(t), :] = (dy[frows(t), :].astype(F32) + through).astype(BF16)

    def between(k, _):
        for half_way, (place, other) in enumerate(((piece, a1t), (a1t, piece))):
            t = 2 * k + half_way
            piece_copy(t, place).wait()

            @pl.when(t + 1 < ftiles)
            def _():
                piece_copy(t + 1, other).start()

            product = mm_nt(place[...], w1[...])
            if half_way:
                through_norm(t - 1)
            else:
                pl.when(k > 0)(lambda: through_norm(t - 1))
            accgu[...] = product
            tick(total + t)
        return 0

    piece_copy(0, piece).start()
    lax.fori_loop(0, ftiles // 2, between, 0)
    through_norm(ftiles - 1)
    accgu[...] = jnp.zeros_like(accgu)

    def front0(i, b):
        c, t = i // tiles, lax.rem(i, tiles)
        a = a0[rows(t), :]
        elementwise(mm(a, w0g[:, cols(c)]), mm(a, w0u[:, cols(c)]), mm_nt(dy[rows(t), :], w0d[cols(c), :]), b)

    def layer0(i, _):
        c, t, b = i // tiles, lax.rem(i, tiles), lax.rem(i, 2)
        accgu[...] += mm(a0t[:, rows(t)], dgu[b])
        accd[...] += mm_tn(act[...], dy[rows(t), :])
        front0(jnp.minimum(i + 1, total - 1), 1 - b)

        @pl.when(t == tiles - 1)
        def _():
            finish(chunks + c)

        tick(total + ftiles + i)
        return 0

    front0(0, 0)
    lax.fori_loop(0, total, layer0, 0)

    def sq_copy(away, mine):
        q = me if mine else lax.rem(me + away, n)
        return pltpu.make_async_remote_copy(
            src_ref=squares.at[0], dst_ref=squares.at[1 + q], send_sem=sq_send.at[away - 1], recv_sem=sq_recv.at[q],
            device_id={AXIS: lax.rem(me + away, n)}, device_id_type=pl.DeviceIdType.MESH)

    end = over - 1 + hops * SPACING
    chances = (ag_lag + 3 * e + 2 * hops * ((pairs + 1 - e) // 2) for e in range(2))
    last = max(end, over + 1 + 2 * (max(chances) - (chunks - 1 + ftiles // 2 + in_layer0)))

    def drain(i, _):
        tick(i)

        @pl.when(i == end)
        def _():
            for away in range(1, n):
                sq_copy(away, True).start()

        return 0

    lax.fori_loop(over, last + 1, drain, 0)
    for away in range(1, n):
        sq_copy(away, True).wait_send()
        sq_copy(away, False).wait_recv()
    squares[pl.ds(1 + me, 1)] = squares[0:1]
    everyone = squares[1]
    for q in range(1, n):
        everyone += squares[1 + q]
    mean = jnp.sum(jnp.sum(everyone, axis=1, keepdims=True), axis=0, keepdims=True) / (6 * d * ff)
    factor_ref[...] = jnp.broadcast_to(jnp.minimum(1.0, 0.5 * lax.rsqrt(mean + 1e-30)), factor_ref.shape)
    me_ref[0] = me
    for pair in range(pairs):
        full_copy(pair).wait()
    own_copy(groups - 1).wait()


def gradients_of(n, x, dy, wg, wu, wd):
    _, tokens, d = x.shape
    _, ff, _ = wd.shape
    chunks, hops = ff // CHUNK, n // 2
    shard_rows = 3 * d // n
    v, dma = pltpu.VMEM, pltpu.SemaphoreType.DMA
    anyspace = pl.BlockSpec(memory_space=pl.ANY)
    return pl.pallas_call(
        functools.partial(gradients_body, n),
        out_shape=(
            jax.ShapeDtypeStruct((chunks, n * shard_rows, CHUNK), BF16),
            jax.ShapeDtypeStruct((chunks, shard_rows, CHUNK), BF16),
            jax.ShapeDtypeStruct((8, 128), F32),
            jax.ShapeDtypeStruct((1,), jnp.int32),
            jax.ShapeDtypeStruct((tokens, 2 * ff), BF16),
        ),
        in_specs=[anyspace] * 5,
        out_specs=(anyspace, anyspace, pl.BlockSpec(memory_space=pltpu.VMEM), pl.BlockSpec(memory_space=pltpu.SMEM), anyspace),
        scratch_shapes=[
            v((tokens, d), BF16), v((d, tokens), BF16), v((tokens, d), BF16), v((d, tokens), BF16),
            v((tokens, d), BF16), v((tokens, d), BF16),
            v((d, ff), BF16), v((d, ff), BF16), v((ff, d), BF16),
            v((d, 2 * ff), BF16), v((2, CHUNK, d), BF16),
            v((TILE, CHUNK), BF16), v((2, TILE, 2 * CHUNK), BF16), v((FTILE, 2 * ff), BF16),
            v((CHUNK, d), F32), v((d, 2 * CHUNK), F32),
            v((chunks + RING, n * shard_rows, CHUNK), BF16),
            v((2, hops, 2, shard_rows, CHUNK), BF16), v((2, hops - 1, shard_rows, CHUNK), BF16),
            v((n + 1, 8, CHUNK), F32),
            dma((9,)), dma((chunks, 2)), dma((2,)), dma((2, hops, 2)), dma((2, hops, 2)), dma((2, hops, 2, 2)), dma((2, hops, 2, 2)),
            dma((n - 1,)), dma((n,)), dma((chunks // 2,)), dma((chunks,)), dma((2,)), dma((2,)),
        ],
        compiler_params=pltpu.CompilerParams(vmem_limit_bytes=VMEM_LIMIT, collective_id=0, has_side_effects=True),
        name="gradients",
    )(x, dy, wg, wu, wd)


def adamw_update(factor, wmv, new, i, at, g):
    g = g.astype(F32) * factor
    w, m, v = (wmv[3 * k + i][at].astype(F32) for k in range(3))
    m = 0.9 * m + 0.1 * g
    v = 0.95 * v + 0.05 * g * g
    w = w - 0.02 * (m * lax.rsqrt(v + 1e-8) + 0.1 * w)
    for k, value in enumerate((w, m, v)):
        new[3 * k + i][at] = value.astype(new[3 * k + i].dtype)


def adamw_gathered_body(n, factor_ref, g_ref, *refs):
    wmv, new = refs[:9], refs[-9:]
    rows_g = g_ref.shape[1] // n
    d = wmv[0].shape[1]
    rd, rf = d // n, CHUNK // n
    update = functools.partial(adamw_update, factor_ref[0:1, 0:1], wmv, new)
    for r in range(n):
        at = r * rows_g
        for i in range(2):
            update(i, (0, slice(r * rd, (r + 1) * rd)), g_ref[0, at + i * rd : at + (i + 1) * rd, :])
        for q in range(d // CHUNK):
            update(2, (0, 0, slice(r * rf, (r + 1) * rf), slice(q * CHUNK, (q + 1) * CHUNK)), g_ref[0, at + 2 * rd + q * rf : at + 2 * rd + (q + 1) * rf, :])


def adamw_shards_body(parts, steps, me_ref, factor_ref, *refs):
    arrays = sum(parts)
    gs, wmv, new, g_all = refs[:arrays], refs[arrays : arrays + 9], refs[-10:-1], refs[-1]
    rd, rf = wmv[0].shape[1], wmv[2].shape[2]
    d = wmv[2].shape[3]
    step = pl.program_id(1)
    update = functools.partial(adamw_update, factor_ref[0:1, 0:1], wmv, new)
    for k, many in enumerate(parts):

        @pl.when((pl.program_id(0) == k) & (step == 0))
        def _():
            first = sum(parts[:k])
            each = g_all.shape[0] // many
            for j in range(many):
                g_all[j * each : (j + 1) * each] = gs[first + j][...]

    for c in range(g_all.shape[0]):
        base = pl.multiple_of(step * rd, rd)
        for i in range(2):
            update(i, (0, slice(None), slice(c * CHUNK, (c + 1) * CHUNK)), g_all[c, pl.ds(base + i * rd * steps, rd), :])
        for p in range(d // CHUNK):
            at = pl.multiple_of(2 * rd * steps + p * rf * steps + step * rf, rf)
            update(2, (0, c, slice(None), slice(p * CHUNK, (p + 1) * CHUNK)), g_all[c, pl.ds(at, rf), :])


def adamw(name, body, grid, prefetch, gs, g_specs, blocks, scratch, share, factor, wmv, before):
    count = int(share * sum(a.size for a in wmv[:3]))
    return pl.pallas_call(
        body,
        grid_spec=pltpu.PrefetchScalarGridSpec(
            num_scalar_prefetch=len(prefetch),
            grid=grid,
            in_specs=[pl.BlockSpec((8, 128), lambda *i: (0, 0)), *g_specs, *blocks, *[pl.BlockSpec(memory_space=pl.ANY)] * len(before)],
            out_specs=blocks,
            scratch_shapes=scratch,
        ),
        out_shape=[jax.ShapeDtypeStruct(a.shape, a.dtype) for a in wmv],
        input_output_aliases={len(prefetch) + 1 + len(gs) + 9 + i: i for i in range(len(before))},
        compiler_params=pltpu.CompilerParams(vmem_limit_bytes=VMEM_LIMIT, dimension_semantics=("arbitrary",) * len(grid)),
        cost_estimate=pl.CostEstimate(flops=400 * count, bytes_accessed=22 * count, transcendentals=count),
        name=name,
    )(*prefetch, factor, *gs, *wmv, *before)


def adamw_gathered(n, layer, lo, hi, g, factor, wmv, before):
    layers, d, ff = wmv[0].shape
    wide = pl.BlockSpec((1, d, CHUNK), lambda c: (layer, 0, c + lo))
    tall = pl.BlockSpec((1, 1, CHUNK, d), lambda c: (layer, c + lo, 0, 0))
    g_spec = pl.BlockSpec((1, g.shape[1], CHUNK), lambda c: (c + lo, 0, 0))
    share = (hi - lo) * CHUNK / (ff * layers)
    return adamw(f"adamw_{layer}_{lo}", functools.partial(adamw_gathered_body, n), (hi - lo,), (), (g,), [g_spec], [wide, wide, tall] * 3, [], share, factor, wmv, before)


def adamw_shards(n, layer, aways, arrays, me, factor, wmv, before):
    def device(k, me):
        away = aways[-1]
        for i, other in enumerate(aways[:-1]):
            away = jnp.where(k == i, other, away)
        return lax.rem(me + away + n, n)

    layers, d, ff = wmv[0].shape
    chunks = ff // CHUNK
    steps = 2 if len(aways) == 1 else 1
    rd, rf = d // n // steps, CHUNK // n // steps
    wide = pl.BlockSpec((1, rd, ff), lambda k, s, me: (layer, device(k, me[0]) * steps + s, 0))
    tall = pl.BlockSpec((1, chunks, rf, d), lambda k, s, me: (layer, 0, device(k, me[0]) * steps + s, 0))
    gs = [g for some in arrays for g in some]
    g_specs = [pl.BlockSpec(g.shape, lambda k, s, me: (0, 0, 0)) for g in gs]
    body = functools.partial(adamw_shards_body, tuple(len(some) for some in arrays), steps)
    scratch = [pltpu.VMEM((chunks, *gs[0].shape[1:]), BF16)]
    return adamw(f"adamw_{layer}_{len(aways)}_{n + aways[0]}", body, (len(aways), steps), (me,), gs, g_specs, [wide, wide, tall] * 3, scratch, len(aways) / (n * layers), factor, wmv, before)


def halves(a, b):
    def copy(a_ref, b_ref, first_ref, second_ref):
        first_ref[...] = a_ref[...]
        second_ref[...] = b_ref[...]

    half = (a.shape[0] // 2, *a.shape[1:])
    zero = (0,) * (a.ndim - 1)
    return pl.pallas_call(
        copy,
        grid=(1,),
        out_shape=[jax.ShapeDtypeStruct(half, a.dtype)] * 2,
        in_specs=[pl.BlockSpec(half, lambda k: (0, *zero)), pl.BlockSpec(half, lambda k: (1, *zero))],
        out_specs=[pl.BlockSpec(half, lambda k: (0, *zero))] * 2,
        compiler_params=pltpu.CompilerParams(vmem_limit_bytes=VMEM_LIMIT),
        name="halves",
    )(a, b)


def solution(mesh):
    n = mesh.shape[AXIS]
    hops = n // 2
    right = [(i, (i + 1) % n) for i in range(n)]
    left = [(i, (i - 1) % n) for i in range(n)]

    def step(x, dy, *wmv):
        full, own, factor, me, _ = gradients_of(n, x, dy, *wmv[:3])
        layers, d, ff = wmv[0].shape
        chunks = ff // CHUNK
        wmv = [a.reshape(layers, chunks, CHUNK, d) if i % 3 == 2 else a for i, a in enumerate(wmv)]

        a, b = lax.ppermute(own, AXIS, right), lax.ppermute(own, AXIS, left)
        most = chunks - chunks // 4 - 1
        new = adamw_gathered(n, 1, 0, most, full, factor, wmv, ())
        (a, b), new = lax.optimization_barrier(((a, b), new))
        ready, some = (0,), (own,)
        for j in range(1, hops):
            ready, some = ready + (-j, j), some + (a, b)
            if j == hops - 1:
                a, b = halves(a, b)
            a, b = lax.ppermute(a, AXIS, right), lax.ppermute(b, AXIS, left)
            if j == 1:
                new = adamw_gathered(n, 1, most, chunks, full, factor, wmv, new)
            take = 1 if j == 1 else 4 if j == 2 else len(ready)
            new = adamw_shards(n, 0, ready[:take], [(g,) for g in some[:take]], me, factor, wmv, new)
            ready, some = ready[take:], some[take:]
            (a, b), new, some = lax.optimization_barrier(((a, b), new, some))
        new = adamw_shards(n, 0, (*ready, hops), [*[(g,) for g in some], (a, b)], me, factor, wmv, new)
        return tuple(new_one.reshape(layers, ff, d) if i % 3 == 2 else new_one for i, new_one in enumerate(new))

    return jax.shard_map(
        step,
        mesh=mesh,
        in_specs=(P(("rep", "dp"), None, None),) * 2 + (P(None, None, None),) * 9,
        out_specs=(P("rep", None, None),) * 9,
        check_vma=False,
    )
```

```python
import functools

import jax
import jax.numpy as jnp
from jax import lax
from jax.experimental import pallas as pl
from jax.experimental.pallas import tpu as pltpu
from jax.sharding import PartitionSpec as P

F32, BF16 = jnp.float32, jnp.bfloat16
AXIS = "dp"
FTILE = 512
TILE = 1024
SPACING = 3
RING = 5
AG_SPACING = 6
CHUNK = 256
VMEM_LIMIT = 67043328


def mm(a, b):
    return jnp.dot(a, b, preferred_element_type=F32)


def mm_nt(a, b):
    return lax.dot_general(a, b, (((1,), (1,)), ((), ())), preferred_element_type=F32)


def mm_tn(a, b):
    return lax.dot_general(a, b, (((0,), (0,)), ((), ())), preferred_element_type=F32)


def sigmoid(x):
    return 0.5 * jnp.tanh(0.5 * x) + 0.5


def normed(wide):
    scale = lax.rsqrt(jnp.mean(wide * wide, -1, keepdims=True) + 1e-6)
    return (wide * scale).astype(BF16)


def gradients_body(n, x_hbm, dy_hbm, wg_hbm, wu_hbm, wd_hbm, full_hbm, own_hbm, factor_ref, me_ref, kept_hbm,
                   a0, a0t, a1, a1t, dy, h1, w0g, w0u, w0d, w1, w1d, act, dgu, piece, accd, accgu, grads, slots, sums, squares, sent,
                   first_sem, w1_sem, w1d_sem, rs_send, rs_recv, ag_send, ag_recv, sq_send, sq_recv, full_sem, own_sem, keep_sem, piece_sem):
    tokens, d = h1.shape
    ff = w0d.shape[0]
    tiles, chunks = tokens // TILE, ff // CHUNK
    groups = 2 * chunks
    hops = n // 2
    shard_rows = grads.shape[1] // n
    half = shard_rows // 2
    me = lax.axis_index(AXIS)
    to = (lax.rem(me + 1, n), lax.rem(me + n - 1, n))

    def rows(t):
        return pl.ds(pl.multiple_of(t * TILE, TILE), TILE)

    def frows(t):
        return pl.ds(pl.multiple_of(t * FTILE, FTILE), FTILE)

    def cols(c):
        return pl.ds(pl.multiple_of(c * CHUNK, CHUNK), CHUNK)

    def shard(away):
        return pl.multiple_of(lax.rem(me + away + n, n) * shard_rows, shard_rows)

    def place(g):
        return jnp.where(g < chunks, g, chunks + lax.rem(g - chunks + RING, RING))

    def remote(src, dst, send, recv, way):
        return pltpu.make_async_remote_copy(src_ref=src, dst_ref=dst, send_sem=send, recv_sem=recv, device_id={AXIS: to[way]}, device_id_type=pl.DeviceIdType.MESH)

    def rs_copy(s, g, way):
        p = lax.rem(g, 2)
        if s == 1:
            part = pl.ds(way * half, half)
            src, dst = grads.at[place(g), pl.ds(shard(hops) + way * half, half)], slots.at[way, 0, p, part]
        else:
            src, dst = sums.at[way, s - 2], slots.at[way, s - 1, p]
        return remote(src, dst, rs_send.at[way, s - 1, p], rs_recv.at[way, s - 1, p], way)

    def rs_add(s, g):
        p = lax.rem(g, 2)
        for way in range(2):
            own = grads[place(g), pl.ds(shard((1 - 2 * way) * (hops + 1 - s)), shard_rows)]
            if s == 2:
                here = slice(way * half, way * half + half)
                there = slice(half - way * half, shard_rows - way * half)
                sums[way, 0, there] = own[there]
                sums[way, 0, here] = (slots[way, 0, p, here].astype(F32) + own[here].astype(F32)).astype(BF16)
            else:
                sums[way, s - 2] = (slots[way, s - 2, p].astype(F32) + own.astype(F32)).astype(BF16)

    def rs_final(g):
        p = lax.rem(g, 2)
        mine = pl.ds(shard(0), shard_rows)
        total = slots[0, hops - 1, p].astype(F32) + slots[1, hops - 1, p].astype(F32) + grads[place(g), mine].astype(F32)
        total = total.astype(BF16)
        grads[place(g), mine] = total
        wide = total.astype(F32)
        squares[...] += jnp.sum((wide * wide).reshape(shard_rows // 8, 8, CHUNK), axis=0)

    def ag_copies(pair, j, whole):
        copies = []
        for b in range(2):
            for way in range(2):
                at = shard((2 * way - 1) * j)
                part = pl.ds(at, shard_rows) if whole else pl.ds(at + way * half, half)
                ref = grads.at[2 * pair + b, part]
                copies.append(remote(ref, ref, ag_send.at[way, j, b, lax.rem(pair, 2)], ag_recv.at[way, j, b, lax.rem(pair, 2)], way))
        return copies

    def full_copy(pair):
        return pltpu.make_async_copy(grads.at[pl.ds(2 * pair, 2)], full_hbm.at[pl.ds(2 * pair, 2)], full_sem.at[pair])

    def own_copy(g):
        return pltpu.make_async_copy(grads.at[place(g), pl.ds(shard(0), shard_rows)], own_hbm.at[g - chunks], own_sem.at[g - chunks])

    pairs = chunks // 2

    total, ftiles = chunks * tiles, tokens // FTILE
    later = total + ftiles
    over = later + total

    ag_lag = -((2 - hops * SPACING) // tiles) + 1
    in_layer0 = (total - 2) // AG_SPACING + 1

    def tick(i):
        def group(s, f):
            step = i - (s - 1) * SPACING - (tiles - 1)
            last_layer = (step >= 0) & (step < total)
            first_layer = (step >= later) & (step < over)
            step = jnp.where(first_layer, step - ftiles, step)
            pl.when((last_layer | first_layer) & (lax.rem(step + tiles * groups, tiles) == 0))(functools.partial(f, step // tiles))

        def hop(s, g):
            if s > 1:
                for way in range(2):
                    rs_copy(s - 1, g, way).wait()
                rs_add(s, g)
            for way in range(2):
                rs_copy(s, g, way).start()

        def final(g):
            for way in range(2):
                rs_copy(hops, g, way).wait()
            rs_final(g)
            pl.when(g > chunks)(lambda: own_copy(g - 1).wait())
            pl.when(g >= chunks)(lambda: own_copy(g).start())

        group(hops + 1, final)
        for s in range(hops, 0, -1):
            group(s, functools.partial(hop, s))

        chance = jnp.where(
            i < total, i // tiles - 1, jnp.where(
                i < later, chunks - 1 + (i - total) // 2, jnp.where(
                    i < over, chunks - 1 + ftiles // 2 + (i - later) // AG_SPACING, chunks - 1 + ftiles // 2 + in_layer0 + (i - over) // 2)))
        due = jnp.where(
            i < total, lax.rem(i, tiles) == 1, jnp.where(
                i < later, lax.rem(i - total, 2) == 1, jnp.where(
                    i < over, lax.rem(i - later, AG_SPACING) == 1, lax.rem(i - over, 2) == 1)))
        chance = chance - ag_lag

        @pl.when(due & (chance >= 0))
        def _():
            odd_pair = (chance > 0) & (lax.rem(chance, 2) == 0)
            e = jnp.where(odd_pair, 1, 0)
            u = jnp.where(odd_pair, (chance - 2) // 2, (chance + 1) // 2)

            def gathering(u, f):
                pair, j = 2 * (u // hops) + e, lax.rem(u + 2 * hops, hops)
                for whole in (True, False):
                    pl.when((u >= 0) & (pair < pairs) & ((j < hops - 1) == whole))(functools.partial(f, pair, j, whole))

            def landed(pair, j, whole):
                for copy in ag_copies(pair, j, whole):
                    copy.wait()
                if not whole:
                    full_copy(pair).start()

            def pass_on(pair, j, whole):
                for copy in ag_copies(pair, j, whole):
                    copy.start()

            gathering(u - 1, landed)
            gathering(u, pass_on)

    def both(c):
        return pl.ds(pl.multiple_of(c * 2 * CHUNK, 2 * CHUNK), 2 * CHUNK)

    def w1_copies(c):
        return (
            pltpu.make_async_copy(wg_hbm.at[1, :, cols(c)], w1.at[:, pl.ds(c * 2 * CHUNK, CHUNK)], w1_sem.at[c, 0]),
            pltpu.make_async_copy(wu_hbm.at[1, :, cols(c)], w1.at[:, pl.ds(c * 2 * CHUNK + CHUNK, CHUNK)], w1_sem.at[c, 1]),
        )

    def w1d_copy(c):
        slot = lax.rem(c, 2)
        return pltpu.make_async_copy(wd_hbm.at[1, cols(c), :], w1d.at[slot], w1d_sem.at[slot])

    squares[...] = jnp.zeros_like(squares)
    barrier = pltpu.get_barrier_semaphore()
    for away in range(1, n):
        pl.semaphore_signal(barrier, inc=1, device_id={AXIS: lax.rem(me + away, n)}, device_id_type=pl.DeviceIdType.MESH)

    first = (
        pltpu.make_async_copy(x_hbm.at[0, pl.ds(0, 2 * FTILE)], h1.at[pl.ds(0, 2 * FTILE)], first_sem.at[0]),
        pltpu.make_async_copy(wg_hbm.at[0], w0g, first_sem.at[1]),
        pltpu.make_async_copy(wu_hbm.at[0], w0u, first_sem.at[2]),
        pltpu.make_async_copy(wd_hbm.at[0], w0d, first_sem.at[3]),
        pltpu.make_async_copy(x_hbm.at[0, pl.ds(2 * FTILE, tokens - 2 * FTILE)], h1.at[pl.ds(2 * FTILE, tokens - 2 * FTILE)], first_sem.at[4]),
        pltpu.make_async_copy(dy_hbm.at[0], dy, first_sem.at[5]),
    )
    for copy in first[:3]:
        copy.start()

    def norm0(t):
        a = normed(h1[frows(t), :].astype(F32))
        a0[frows(t), :] = a
        a0t[:, frows(t)] = a.T

    def expand(t):
        a = a0[frows(t), :]
        for c in range(chunks):
            s = pl.ds(c * CHUNK, CHUNK)
            gate, up = mm(a, w0g[:, s]), mm(a, w0u[:, s])
            piece[:, pl.ds(pl.multiple_of(lax.rem(t, 2) * ff + c * CHUNK, CHUNK), CHUNK)] = (gate * sigmoid(gate) * up).astype(BF16)

    def contract(t):
        out = mm(piece[:, pl.ds(pl.multiple_of(lax.rem(t, 2) * ff, CHUNK), ff)], w0d[...])
        h = (h1[frows(t), :].astype(F32) + out.astype(BF16).astype(F32)).astype(BF16)
        h1[frows(t), :] = h
        a = normed(h.astype(F32))
        a1[frows(t), :] = a
        a1t[:, frows(t)] = a.T

    first[0].wait()
    for copy in first[3:5]:
        copy.start()
    norm0(0)
    norm0(1)
    first[1].wait()
    first[2].wait()
    for copy in first[5:]:
        copy.start()
    for c in range(chunks):
        for copy in w1_copies(c):
            copy.start()
        if c < 2:
            w1d_copy(c).start()
    expand(0)
    accd[...] = jnp.zeros_like(accd)
    accgu[...] = jnp.zeros_like(accgu)
    first[3].wait()
    first[4].wait()

    def forward(t, _):
        contract(t)
        expand(t + 1)
        norm0(jnp.minimum(t + 2, ftiles - 1))
        return 0

    lax.fori_loop(0, ftiles - 1, forward, 0)
    contract(ftiles - 1)
    first[5].wait()
    pl.semaphore_wait(barrier, n - 1)

    def elementwise(gate, up, dact, b):
        s = sigmoid(gate)
        p = gate * s
        act[...] = (p * up).astype(BF16)
        dact = dact.astype(BF16).astype(F32)
        dgu[b, :, CHUNK:] = (dact * p).astype(BF16)
        dgu[b, :, :CHUNK] = (dact * up * (s + p * (1.0 - s))).astype(BF16)

    def finish(g):
        rd, rf, to_group = d // n, CHUNK // n, place(g)
        for r in range(n):
            at = r * shard_rows
            grads[to_group, at : at + rd, :] = accgu[r * rd : (r + 1) * rd, :CHUNK].astype(BF16)
            grads[to_group, at + rd : at + 2 * rd, :] = accgu[r * rd : (r + 1) * rd, CHUNK:].astype(BF16)
            for q in range(d // CHUNK):
                grads[to_group, at + 2 * rd + q * rf : at + 2 * rd + (q + 1) * rf, :] = accd[r * rf : (r + 1) * rf, q * CHUNK : (q + 1) * CHUNK].astype(BF16)
        accd[...] = jnp.zeros_like(accd)
        accgu[...] = jnp.zeros_like(accgu)

    def kept(i):
        c, t, b = i // tiles, lax.rem(i, tiles), lax.rem(i, 2)
        return pltpu.make_async_copy(dgu.at[b], kept_hbm.at[rows(t), both(c)], keep_sem.at[b])

    def front1(i, b):
        c, t = i // tiles, lax.rem(i, tiles)
        a = a1[rows(t), :]
        w = w1[:, both(c)]
        elementwise(mm(a, w[:, :CHUNK]), mm(a, w[:, CHUNK:]), mm_nt(dy[rows(t), :], w1d[lax.rem(c, 2)]), b)

    def layer1(i, _):
        c, t, b = i // tiles, lax.rem(i, tiles), lax.rem(i, 2)

        @pl.when((t == tiles - 1) & (c + 1 < chunks))
        def _():
            for copy in w1_copies(c + 1):
                copy.wait()
            w1d_copy(c + 1).wait()

        kept(i).start()

        @pl.when(i > 0)
        def _():
            kept(i - 1).wait()

        accgu[...] += mm(a1t[:, rows(t)], dgu[b])
        accd[...] += mm_tn(act[...], dy[rows(t), :])
        front1(jnp.minimum(i + 1, total - 1), 1 - b)

        @pl.when(t == tiles - 1)
        def _():
            finish(c)

            @pl.when(c + 2 < chunks)
            def _():
                w1d_copy(c + 2).start()

        tick(i)
        return 0

    for copy in w1_copies(0):
        copy.wait()
    w1d_copy(0).wait()
    front1(0, 0)
    lax.fori_loop(0, total, layer1, 0)
    kept(total - 1).wait()

    def piece_copy(t, place):
        return pltpu.make_async_copy(kept_hbm.at[frows(t), :], place, piece_sem.at[lax.rem(t, 2)])

    def through_norm(t):
        by_a = accgu[...].astype(BF16).astype(F32)
        wide = h1[frows(t), :].astype(F32)
        scale = lax.rsqrt(jnp.mean(wide * wide, -1, keepdims=True) + 1e-6)
        along = jnp.sum(by_a * wide, -1, keepdims=True) * (scale * scale * scale / d)
        through = (by_a * scale - wide * along).astype(BF16).astype(F32)
        dy[frows(t), :] = (dy[frows(t), :].astype(F32) + through).astype(BF16)

    def between(k, _):
        for half_way, (place, other) in enumerate(((piece, a1t), (a1t, piece))):
            t = 2 * k + half_way
            piece_copy(t, place).wait()

            @pl.when(t + 1 < ftiles)
            def _():
                piece_copy(t + 1, other).start()

            product = mm_nt(place[...], w1[...])
            if half_way:
                through_norm(t - 1)
            else:
                pl.when(k > 0)(lambda: through_norm(t - 1))
            accgu[...] = product
            tick(total + t)
        return 0

    piece_copy(0, piece).start()
    lax.fori_loop(0, ftiles // 2, between, 0)
    through_norm(ftiles - 1)
    accgu[...] = jnp.zeros_like(accgu)

    def front0(i, b):
        c, t = i // tiles, lax.rem(i, tiles)
        a = a0[rows(t), :]
        elementwise(mm(a, w0g[:, cols(c)]), mm(a, w0u[:, cols(c)]), mm_nt(dy[rows(t), :], w0d[cols(c), :]), b)

    def layer0(i, _):
        c, t, b = i // tiles, lax.rem(i, tiles), lax.rem(i, 2)
        accgu[...] += mm(a0t[:, rows(t)], dgu[b])
        accd[...] += mm_tn(act[...], dy[rows(t), :])
        front0(jnp.minimum(i + 1, total - 1), 1 - b)

        @pl.when(t == tiles - 1)
        def _():
            finish(chunks + c)

        tick(total + ftiles + i)
        return 0

    front0(0, 0)
    lax.fori_loop(0, total, layer0, 0)

    def sq_copy(away, mine):
        q = me if mine else lax.rem(me + away, n)
        return pltpu.make_async_remote_copy(
            src_ref=sent.at[0], dst_ref=sent.at[1 + q], send_sem=sq_send.at[away - 1], recv_sem=sq_recv.at[q],
            device_id={AXIS: lax.rem(me + away, n)}, device_id_type=pl.DeviceIdType.MESH)

    end = over - 1 + hops * SPACING
    chances = (ag_lag + 2 * hops * ((pairs + 1) // 2) - 1, ag_lag + 2 * hops * (pairs // 2) + 2)
    last = max(end, over + 1 + 2 * (max(chances) - (chunks - 1 + ftiles // 2 + in_layer0)))

    def drain(i, _):
        tick(i)

        @pl.when(i == end)
        def _():
            sent[0] = jnp.sum(squares[...], axis=0, keepdims=True)
            for away in range(1, n):
                sq_copy(away, True).start()

        return 0

    lax.fori_loop(over, last + 1, drain, 0)
    for away in range(1, n):
        sq_copy(away, True).wait_send()
        sq_copy(away, False).wait_recv()
    sent[pl.ds(1 + me, 1)] = sent[0:1]
    everyone = sent[1]
    for q in range(1, n):
        everyone += sent[1 + q]
    mean = jnp.sum(everyone, axis=1, keepdims=True) / (6 * d * ff)
    factor_ref[...] = jnp.broadcast_to(jnp.minimum(1.0, 0.5 * lax.rsqrt(mean + 1e-30)), factor_ref.shape)
    me_ref[0] = me
    for pair in range(pairs):
        full_copy(pair).wait()
    own_copy(groups - 1).wait()


def gradients_of(n, x, dy, wg, wu, wd):
    _, tokens, d = x.shape
    _, ff, _ = wd.shape
    chunks, hops = ff // CHUNK, n // 2
    shard_rows = 3 * d // n
    v, dma = pltpu.VMEM, pltpu.SemaphoreType.DMA
    anyspace = pl.BlockSpec(memory_space=pl.ANY)
    return pl.pallas_call(
        functools.partial(gradients_body, n),
        out_shape=(
            jax.ShapeDtypeStruct((chunks, n * shard_rows, CHUNK), BF16),
            jax.ShapeDtypeStruct((chunks, shard_rows, CHUNK), BF16),
            jax.ShapeDtypeStruct((8, 128), F32),
            jax.ShapeDtypeStruct((1,), jnp.int32),
            jax.ShapeDtypeStruct((tokens, 2 * ff), BF16),
        ),
        in_specs=[anyspace] * 5,
        out_specs=(anyspace, anyspace, pl.BlockSpec(memory_space=pltpu.VMEM), pl.BlockSpec(memory_space=pltpu.SMEM), anyspace),
        scratch_shapes=[
            v((tokens, d), BF16), v((d, tokens), BF16), v((tokens, d), BF16), v((d, tokens), BF16),
            v((tokens, d), BF16), v((tokens, d), BF16),
            v((d, ff), BF16), v((d, ff), BF16), v((ff, d), BF16),
            v((d, 2 * ff), BF16), v((2, CHUNK, d), BF16),
            v((TILE, CHUNK), BF16), v((2, TILE, 2 * CHUNK), BF16), v((FTILE, 2 * ff), BF16),
            v((CHUNK, d), F32), v((d, 2 * CHUNK), F32),
            v((chunks + RING, n * shard_rows, CHUNK), BF16),
            v((2, hops, 2, shard_rows, CHUNK), BF16), v((2, hops - 1, shard_rows, CHUNK), BF16),
            v((8, CHUNK), F32), v((n + 1, 1, CHUNK), F32),
            dma((6,)), dma((chunks, 2)), dma((2,)), dma((2, hops, 2)), dma((2, hops, 2)), dma((2, hops, 2, 2)), dma((2, hops, 2, 2)),
            dma((n - 1,)), dma((n,)), dma((chunks // 2,)), dma((chunks,)), dma((2,)), dma((2,)),
        ],
        compiler_params=pltpu.CompilerParams(vmem_limit_bytes=VMEM_LIMIT, collective_id=0, has_side_effects=True),
        name="gradients",
    )(x, dy, wg, wu, wd)


def adamw_update(factor, wmv, new, i, at, g):
    g = g.astype(F32) * factor
    w, m, v = (wmv[3 * k + i][at].astype(F32) for k in range(3))
    m = 0.9 * m + 0.1 * g
    v = 0.95 * v + 0.05 * g * g
    w = w - 0.02 * (m * lax.rsqrt(v + 1e-8) + 0.1 * w)
    for k, value in enumerate((w, m, v)):
        new[3 * k + i][at] = value.astype(new[3 * k + i].dtype)


def adamw_gathered_body(n, factor_ref, g_ref, *refs):
    wmv, new = refs[:9], refs[-9:]
    rows_g = g_ref.shape[1] // n
    d = wmv[0].shape[1]
    rd, rf = d // n, CHUNK // n
    update = functools.partial(adamw_update, factor_ref[0:1, 0:1], wmv, new)
    for r in range(n):
        at = r * rows_g
        for i in range(2):
            update(i, (0, slice(r * rd, (r + 1) * rd)), g_ref[0, at + i * rd : at + (i + 1) * rd, :])
        for q in range(d // CHUNK):
            update(2, (0, 0, slice(r * rf, (r + 1) * rf), slice(q * CHUNK, (q + 1) * CHUNK)), g_ref[0, at + 2 * rd + q * rf : at + 2 * rd + (q + 1) * rf, :])


def adamw_shards_body(parts, steps, me_ref, factor_ref, *refs):
    arrays = sum(parts)
    gs, wmv, new, g_all = refs[:arrays], refs[arrays : arrays + 9], refs[-10:-1], refs[-1]
    rd, rf = wmv[0].shape[1], wmv[2].shape[2]
    d = wmv[2].shape[3]
    step = pl.program_id(1)
    update = functools.partial(adamw_update, factor_ref[0:1, 0:1], wmv, new)
    for k, many in enumerate(parts):

        @pl.when((pl.program_id(0) == k) & (step == 0))
        def _():
            first = sum(parts[:k])
            each = g_all.shape[0] // many
            for j in range(many):
                g_all[j * each : (j + 1) * each] = gs[first + j][...]

    for c in range(g_all.shape[0]):
        base = pl.multiple_of(step * rd, rd)
        for i in range(2):
            update(i, (0, slice(None), slice(c * CHUNK, (c + 1) * CHUNK)), g_all[c, pl.ds(base + i * rd * steps, rd), :])
        for p in range(d // CHUNK):
            at = pl.multiple_of(2 * rd * steps + p * rf * steps + step * rf, rf)
            update(2, (0, c, slice(None), slice(p * CHUNK, (p + 1) * CHUNK)), g_all[c, pl.ds(at, rf), :])


def adamw(name, body, grid, prefetch, gs, g_specs, blocks, scratch, share, factor, wmv, before):
    count = int(share * sum(a.size for a in wmv[:3]))
    return pl.pallas_call(
        body,
        grid_spec=pltpu.PrefetchScalarGridSpec(
            num_scalar_prefetch=len(prefetch),
            grid=grid,
            in_specs=[pl.BlockSpec((8, 128), lambda *i: (0, 0)), *g_specs, *blocks, *[pl.BlockSpec(memory_space=pl.ANY)] * len(before)],
            out_specs=blocks,
            scratch_shapes=scratch,
        ),
        out_shape=[jax.ShapeDtypeStruct(a.shape, a.dtype) for a in wmv],
        input_output_aliases={len(prefetch) + 1 + len(gs) + 9 + i: i for i in range(len(before))},
        compiler_params=pltpu.CompilerParams(vmem_limit_bytes=VMEM_LIMIT, dimension_semantics=("arbitrary",) * len(grid)),
        cost_estimate=pl.CostEstimate(flops=400 * count, bytes_accessed=22 * count, transcendentals=count),
        name=name,
    )(*prefetch, factor, *gs, *wmv, *before)


def adamw_gathered(n, layer, lo, hi, g, factor, wmv, before):
    layers, d, ff = wmv[0].shape
    wide = pl.BlockSpec((1, d, CHUNK), lambda c: (layer, 0, c + lo))
    tall = pl.BlockSpec((1, 1, CHUNK, d), lambda c: (layer, c + lo, 0, 0))
    g_spec = pl.BlockSpec((1, g.shape[1], CHUNK), lambda c: (c + lo, 0, 0))
    share = (hi - lo) * CHUNK / (ff * layers)
    return adamw(f"adamw_{layer}_{lo}", functools.partial(adamw_gathered_body, n), (hi - lo,), (), (g,), [g_spec], [wide, wide, tall] * 3, [], share, factor, wmv, before)


def adamw_shards(n, layer, aways, arrays, me, factor, wmv, before):
    def device(k, me):
        away = aways[-1]
        for i, other in enumerate(aways[:-1]):
            away = jnp.where(k == i, other, away)
        return lax.rem(me + away + n, n)

    layers, d, ff = wmv[0].shape
    chunks = ff // CHUNK
    steps = 2 if len(aways) == 1 else 1
    rd, rf = d // n // steps, CHUNK // n // steps
    wide = pl.BlockSpec((1, rd, ff), lambda k, s, me: (layer, device(k, me[0]) * steps + s, 0))
    tall = pl.BlockSpec((1, chunks, rf, d), lambda k, s, me: (layer, 0, device(k, me[0]) * steps + s, 0))
    gs = [g for some in arrays for g in some]
    g_specs = [pl.BlockSpec(g.shape, lambda k, s, me: (0, 0, 0)) for g in gs]
    body = functools.partial(adamw_shards_body, tuple(len(some) for some in arrays), steps)
    scratch = [pltpu.VMEM((chunks, *gs[0].shape[1:]), BF16)]
    return adamw(f"adamw_{layer}_{len(aways)}_{n + aways[0]}", body, (len(aways), steps), (me,), gs, g_specs, [wide, wide, tall] * 3, scratch, len(aways) / (n * layers), factor, wmv, before)


def halves(a, b):
    def copy(a_ref, b_ref, first_ref, second_ref):
        first_ref[...] = a_ref[...]
        second_ref[...] = b_ref[...]

    half = (a.shape[0] // 2, *a.shape[1:])
    zero = (0,) * (a.ndim - 1)
    return pl.pallas_call(
        copy,
        grid=(1,),
        out_shape=[jax.ShapeDtypeStruct(half, a.dtype)] * 2,
        in_specs=[pl.BlockSpec(half, lambda k: (0, *zero)), pl.BlockSpec(half, lambda k: (1, *zero))],
        out_specs=[pl.BlockSpec(half, lambda k: (0, *zero))] * 2,
        compiler_params=pltpu.CompilerParams(vmem_limit_bytes=VMEM_LIMIT),
        name="halves",
    )(a, b)


def solution(mesh):
    n = mesh.shape[AXIS]
    hops = n // 2
    right = [(i, (i + 1) % n) for i in range(n)]
    left = [(i, (i - 1) % n) for i in range(n)]

    def step(x, dy, *wmv):
        full, own, factor, me, _ = gradients_of(n, x, dy, *wmv[:3])
        layers, d, ff = wmv[0].shape
        chunks = ff // CHUNK
        wmv = [a.reshape(layers, chunks, CHUNK, d) if i % 3 == 2 else a for i, a in enumerate(wmv)]

        a, b = lax.ppermute(own, AXIS, right), lax.ppermute(own, AXIS, left)
        most = chunks - chunks // 4 - 1
        new = adamw_gathered(n, 1, 0, most, full, factor, wmv, ())
        (a, b), new = lax.optimization_barrier(((a, b), new))
        ready, some = (0,), (own,)
        for j in range(1, hops):
            ready, some = ready + (-j, j), some + (a, b)
            if j == hops - 1:
                a, b = halves(a, b)
            a, b = lax.ppermute(a, AXIS, right), lax.ppermute(b, AXIS, left)
            if j == 1:
                new = adamw_gathered(n, 1, most, chunks, full, factor, wmv, new)
            take = 1 if j == 1 else 4 if j == 2 else len(ready)
            new = adamw_shards(n, 0, ready[:take], [(g,) for g in some[:take]], me, factor, wmv, new)
            ready, some = ready[take:], some[take:]
            (a, b), new, some = lax.optimization_barrier(((a, b), new, some))
        new = adamw_shards(n, 0, (*ready, hops), [*[(g,) for g in some], (a, b)], me, factor, wmv, new)
        return tuple(new_one.reshape(layers, ff, d) if i % 3 == 2 else new_one for i, new_one in enumerate(new))

    return jax.shard_map(
        step,
        mesh=mesh,
        in_specs=(P(("rep", "dp"), None, None),) * 2 + (P(None, None, None),) * 9,
        out_specs=(P("rep", None, None),) * 9,
        check_vma=False,
    )
```
